32 devices in a mesh: rep: 4 (over x, core), ep: 4 (over z), grp: 2 (over y).
Axes of the slice: x: 2, y: 2, z: 4, core: 2. Of those that a mesh axis runs over, the one named last changes fastest.
Arguments:
- tokens: bfloat16 [4096, 2048], P(('rep', 'ep', 'grp')), may hold values from -6 to 6
- grad_out: bfloat16 [4096, 2048], P(('rep', 'ep', 'grp')), may hold values from -6 to 6
- expert_ids: int32 [4096, 2], P(('rep', 'ep', 'grp')), may hold values from 0 to 7, as said below
- combine: bfloat16 [4096, 2], P(('rep', 'ep', 'grp')), may hold values from 0.099609375 to 1
- weights: bfloat16 [2048, 3, 7168], P('grp', None, 'ep'), may hold values from -0.125 to 0.125
Outputs:
- grad_tokens: bfloat16 [4096, 2048], P(('rep', 'ep', 'grp'))
- grad_combine: float32 [4096, 2], P(('rep', 'ep', 'grp'))
- grad_weights: float32 [2048, 3, 7168], P(('rep', 'grp'), None, 'ep')
The draws below stay inside these ranges and needn't reach their ends.
Inputs may be any that keep to these rules, and one draw needn't show every extreme that they name: `expert_ids`: each token names 2 different experts, at most one of them below 1. No expert below 1 is named by more than 4 tokens of one device, and each of them is named by exactly 4 tokens of some device.
All inputs are finite; a program needn't handle non-finite values.
Results may differ from the reference program's by a relative error of at most 0.0085.
Values may be sent and summed in bfloat16 or wider, within the bound.
No kernel may reach another device: no remote copies, remote signals or barrier semaphores. Data moves between devices by JAX's collectives and lax.ppermute only.
A program may use at most 128 MiB of HBM per device.

```python
import jax
import jax.numpy as jnp
from jax import lax

D = 2048
FF = 7168
EXPERTS = 8
TOPK = 2
FLIGHT = 1
TOK_DEV = 128
CAP = 4
TOKENS = 4096
N_REP = 4
N_EP = 4
N_GRP = 2
DEVICES = 32


def draw_expert_ids(key, part):
    keys = jax.random.split(jax.random.fold_in(key, 7001), 6)
    blocks = DEVICES
    rows = TOK_DEV
    scores = jax.random.randint(keys[0], (blocks, rows), 0, 1 << 20) * rows + jnp.arange(rows, dtype=jnp.int32)[None, :]
    order = jnp.argsort(scores, axis=1)
    rank = jnp.argsort(order, axis=1).astype(jnp.int32)
    counts = jax.random.randint(keys[1], (blocks, FLIGHT), 0, CAP + 1)
    forced = jax.random.randint(keys[2], (FLIGHT,), 0, blocks)
    block_index = jnp.arange(blocks, dtype=jnp.int32)
    counts = jnp.where(block_index[:, None] == forced[None, :], CAP, counts).astype(jnp.int32)
    bounds = jnp.cumsum(counts, axis=1)
    lower = bounds - counts
    hits = (rank[:, :, None] >= lower[:, None, :]) & (rank[:, :, None] < bounds[:, None, :])
    hit_int = hits.astype(jnp.int32)
    chosen = jnp.sum(hit_int, axis=2) > 0
    flight_id = jnp.sum(hit_int * jnp.arange(FLIGHT, dtype=jnp.int32)[None, None, :], axis=2)
    others = EXPERTS - FLIGHT
    first = jax.random.randint(keys[3], (blocks, rows), 0, others)
    second = (first + jax.random.randint(keys[4], (blocks, rows), 1, others)) % others
    first = first + FLIGHT
    second = second + FLIGHT
    column_a = jnp.where(chosen, flight_id, first)
    column_b = jnp.where(chosen, first, second)
    flipped = jax.random.randint(keys[5], (blocks, rows), 0, 2) == 1
    left = jnp.where(flipped, column_b, column_a)
    right = jnp.where(flipped, column_a, column_b)
    return jnp.stack([left, right], axis=-1).reshape(TOKENS, TOPK).astype(jnp.int32)


def shard_levels(key, extent, shards, smallest, largest):
    gain = 1.0
    for axis_at, shards_of in shards:
        heights = jax.random.uniform(jax.random.fold_in(jax.random.fold_in(key, 6), axis_at), (shards_of,), jnp.float32, smallest / len(shards), largest / len(shards))
        gain = gain * jnp.repeat(jnp.exp(heights), extent[axis_at] // shards_of).reshape((-1,) + (1,) * (len(extent) - 1 - axis_at))
    return gain


def gaussian(key, shape, spread, most, pieces=(), kind=jnp.bfloat16):
    gain = shard_levels(key, shape, pieces, -0.22, 0.18) if pieces else 1.0
    drawn = jax.random.normal(key, shape, jnp.float32) * spread * gain
    return jnp.minimum(jnp.maximum(drawn, -most), most).astype(kind)


def setup_inputs(seed: int = 0) -> dict:
    arg_keys = jax.random.split(jax.random.key(seed), 6)
    tokens = gaussian(arg_keys[0], (TOKENS, D), 1.0, 6.0, ((0, 32),))
    grad_out = gaussian(arg_keys[1], (TOKENS, D), 1.0, 6.0, ((0, 32),))
    expert_ids = draw_expert_ids(jax.random.fold_in(arg_keys[5], 71), 0)
    combine = jnp.clip(0.099609375 + 0.9003906 * jax.random.uniform(arg_keys[3], (TOKENS, TOPK), jnp.float32) ** shard_levels(arg_keys[3], (TOKENS, TOPK), ((0, 32),), -0.2, 0.2), 0.099609375, 1.0).astype(jnp.bfloat16)
    weights = gaussian(arg_keys[4], (D, 3, FLIGHT * FF), D ** -0.5, 0.125, ((0, 2), (2, 4)))
    return dict(tokens=tokens, grad_out=grad_out, expert_ids=expert_ids, combine=combine, weights=weights)


def route_slots(routing, gate_vals, in_flight, capacity):
    experts = jnp.arange(in_flight, dtype=jnp.int32)
    matches = (routing[None, :, :] == experts[:, None, None]).astype(jnp.float32)
    assigned = jnp.sum(matches, axis=2)
    combined = jnp.sum(matches * gate_vals.astype(jnp.float32)[None, :, :], axis=2)
    before = jnp.cumsum(assigned, axis=1) - assigned
    slot_index = jnp.arange(capacity, dtype=jnp.float32)
    slot_map = (before[:, None, :] == slot_index[None, :, None]).astype(jnp.float32) * assigned[:, None, :]
    return matches, combined, slot_map


def rounded(values):
    return lax.optimization_barrier(values.astype(jnp.bfloat16)).astype(jnp.float32)


def reference(tokens, grad_out, expert_ids, combine, weights):
    quarter = N_EP // FLIGHT
    hidden = FF // quarter
    slot_total = N_EP * CAP
    highest = lax.Precision.HIGHEST

    def regroup(values):
        trailing = values.shape[1:]
        shaped = values.reshape((N_REP, N_EP, N_GRP, TOK_DEV) + trailing)
        return jnp.moveaxis(shaped, 2, 1)

    def ungroup(values):
        trailing = values.shape[4:]
        reordered = jnp.moveaxis(values, 1, 2)
        return reordered.reshape((N_REP * N_EP * N_GRP * TOK_DEV,) + trailing)

    split_weights = weights.reshape(D, 3, FLIGHT, FF)

    def one_group(accumulated, blocks):
        token_block, grad_block, routing, gate_vals = blocks
        matches, combined, slot_map = jax.vmap(lambda ids_one, vals_one: route_slots(ids_one, vals_one, FLIGHT, CAP))(routing, gate_vals)
        sent_rows = jnp.einsum("sfct,std->fscd", slot_map, token_block.astype(jnp.float32), precision=highest).astype(jnp.bfloat16)
        sent_grads = jnp.einsum("sfct,std->fscd", slot_map, grad_block.astype(jnp.float32), precision=highest).astype(jnp.bfloat16)
        sent_scale = jnp.einsum("sfct,sft->fsc", slot_map, combined, precision=highest)
        grad_tok = jnp.zeros((N_EP, TOK_DEV, D), jnp.float32)
        per_list = []
        term_list = []
        for expert in range(FLIGHT):
            token_rows = sent_rows[expert].reshape(slot_total, D)
            grad_rows = sent_grads[expert].reshape(slot_total, D)
            row_scale = sent_scale[expert].reshape(slot_total, 1)
            gate_pre = jnp.dot(token_rows, split_weights[:, 0, expert], preferred_element_type=jnp.float32)
            up_pre = jnp.dot(token_rows, split_weights[:, 1, expert], preferred_element_type=jnp.float32)
            down_back = jnp.dot(grad_rows, split_weights[:, 2, expert], preferred_element_type=jnp.float32)
            sigmoid_gate = jax.nn.sigmoid(gate_pre)
            activated = gate_pre * sigmoid_gate
            hid_value = activated * up_pre
            hid_grad = row_scale * down_back
            grad_gate = (hid_grad * up_pre * sigmoid_gate * (1.0 + gate_pre * (1.0 - sigmoid_gate))).astype(jnp.bfloat16)
            grad_up = (hid_grad * activated).astype(jnp.bfloat16)
            scaled_hid = (row_scale * hid_value).astype(jnp.bfloat16)
            gate_up_grad = jnp.stack([grad_gate, grad_up], axis=1).astype(jnp.float32)
            sliced_grad = gate_up_grad.reshape(slot_total, 2, quarter, hidden)
            sliced_weight = split_weights[:, :2, expert].astype(jnp.float32).reshape(D, 2, quarter, hidden)
            partial_x = jnp.einsum("rkqh,dkqh->qrd", sliced_grad, sliced_weight)
            summed_x = jnp.sum(rounded(partial_x), axis=0)
            partial_c = jnp.sum((hid_value * down_back).reshape(slot_total, quarter, hidden), axis=2)
            summed_c = jnp.sum(rounded(partial_c), axis=1)
            grad_tok = grad_tok + jnp.einsum("sct,scd->std", slot_map[:, expert], summed_x.reshape(N_EP, CAP, D), precision=highest)
            per_list.append(jnp.einsum("sct,sc->st", slot_map[:, expert], summed_c.reshape(N_EP, CAP), precision=highest))
            gate_up_term = jnp.einsum("rd,rkf->dkf", token_rows.astype(jnp.float32), gate_up_grad)
            down_term = jnp.dot(grad_rows.T, scaled_hid, preferred_element_type=jnp.float32)
            term_list.append(jnp.concatenate([gate_up_term, down_term[:, None, :]], axis=1))
        group_term = jnp.stack(term_list, axis=2)
        per_token = jnp.stack(per_list, axis=1)
        grad_gates = jnp.sum(matches * per_token[:, :, :, None], axis=1)
        return accumulated + group_term, (grad_tok.astype(jnp.bfloat16), grad_gates)

    def one_rep(total, rep_blocks):
        start = jnp.zeros((D, 3, FLIGHT, FF), jnp.float32)
        rep_sum, outputs = lax.scan(one_group, start, rep_blocks)
        return total + rounded(rep_sum), outputs

    initial = jnp.zeros((D, 3, FLIGHT, FF), jnp.float32)
    inputs_group = (regroup(tokens), regroup(grad_out), regroup(expert_ids), regroup(combine))
    accumulated, outputs_group = lax.scan(one_rep, initial, inputs_group)
    grad_tokens = ungroup(outputs_group[0])
    grad_combine = ungroup(outputs_group[1])
    return grad_tokens, grad_combine, accumulated.reshape(D, 3, FLIGHT * FF)
```

```python
import functools

import jax
import jax.numpy as jnp
from jax import lax
from jax.experimental import pallas as pl
from jax.experimental.pallas import tpu as pltpu
from jax.sharding import PartitionSpec as P

CAP = 4
PACK = 2 * CAP
LANES = 128
BF = jnp.bfloat16
F32 = jnp.float32


def tile_of(extent, most):
    for tile in range(most, 0, -LANES):
        if tile % LANES == 0 and extent % tile == 0:
            return tile
    return extent


def iota(shape, axis):
    return lax.broadcasted_iota(jnp.int32, shape, axis)


def slots(ids):
    tokens = ids.shape[1]
    named = jnp.sum((ids == 0).astype(F32), axis=0, keepdims=True)
    earlier = (iota((tokens, tokens), 0) < iota((tokens, tokens), 1)).astype(BF)
    wide = jnp.broadcast_to(named, (PACK, tokens))
    before = jnp.dot(wide.astype(BF), earlier, preferred_element_type=F32)
    slot = (iota((PACK, tokens), 0) % CAP).astype(F32)
    return jnp.where(before == slot, wide, 0.0)


def pack_kernel(ids_ref, comb_ref, tok_ref, out_ref, rows_ref, cols_ref, *, grp_size, owners):
    ids = ids_ref[...]
    both = slots(ids)
    model_width = tok_ref.shape[1]
    tokens = ids.shape[1]
    half = model_width // grp_size
    upper = iota((PACK, tokens), 0) < CAP
    first = jnp.where(upper, both, 0.0).astype(BF)
    second = jnp.where(upper, 0.0, both).astype(BF)
    packed = (
        jnp.dot(first, tok_ref[...], preferred_element_type=F32)
        + jnp.dot(second, out_ref[...], preferred_element_type=F32)
    ).astype(BF)
    chosen = jnp.sum(
        jnp.where(ids == 0, comb_ref[...].astype(F32), 0.0), axis=0, keepdims=True
    )
    scale = jnp.sum(both * chosen, axis=1, keepdims=True)
    scale = jnp.broadcast_to(scale, (PACK, LANES)).astype(BF)
    for peer in range(rows_ref.shape[0]):
        side = peer % grp_size
        rows_ref[peer, :, :half] = packed[:, side * half : (side + 1) * half]
        rows_ref[peer, :, half:] = scale
    width = model_width // owners
    spread = cols_ref.shape[0] // owners
    for owner in range(owners):
        rep, grp = owner // grp_size, owner % grp_size
        for at in range(spread):
            cols_ref[(rep * spread + at) * grp_size + grp] = packed[
                :, owner * width : (owner + 1) * width
            ]


def forward_kernel(recv_ref, w_ref, own_ref, send_ref, scale_ref, rows_ref):
    depth = w_ref.shape[1]

    @pl.when(pl.program_id(0) == 0)
    def _():
        peers = recv_ref.shape[0] // PACK
        block = 8 if peers % 8 == 0 else peers
        many = block * CAP
        row, col = iota((many, block * PACK), 0), iota((many, block * PACK), 1)
        source = row // CAP * PACK + row % CAP
        take_x = (col == source).astype(BF)
        take_y = (col == source + CAP).astype(BF)
        for at in range(peers // block):
            piece = recv_ref[at * block * PACK : (at + 1) * block * PACK, :]
            xr = jnp.dot(take_x, piece, preferred_element_type=F32)
            yr = jnp.dot(take_y, piece[:, :depth], preferred_element_type=F32)
            here = pl.ds(at * many, many)
            rows_ref[0, here, :] = xr[:, :depth].astype(BF)
            rows_ref[1, here, :] = yr.astype(BF)
            scale_ref[here, :] = xr[:, depth:]

    for k in range(3):
        part = jnp.dot(rows_ref[k // 2], w_ref[k], preferred_element_type=F32)
        own_ref[k] = part
        send_ref[k] = part.astype(BF)


def hidden_kernel(own_ref, other_ref, scale_ref, w_ref, hid_ref, back_ref, px_ref, pc_ref):
    step = pl.program_id(0)

    @pl.when(step == 0)
    def _():
        px_ref[...] = jnp.zeros_like(px_ref)
        pc_ref[...] = jnp.zeros_like(pc_ref)

    a = own_ref[0] + other_ref[0].astype(F32)
    b = own_ref[1] + other_ref[1].astype(F32)
    back = own_ref[2] + other_ref[2].astype(F32)
    cr = scale_ref[:, :1]
    sig = jax.nn.sigmoid(a)
    act = a * sig
    h = act * b
    dh = cr * back
    da = (dh * b * sig * (1.0 + a * (1.0 - sig))).astype(BF)
    db = (dh * act).astype(BF)
    hid_ref[0] = da
    hid_ref[1] = db
    hid_ref[2] = (cr * h).astype(BF)
    contract = (((1,), (1,)), ((), ()))
    px_ref[...] += lax.dot_general(
        da, w_ref[0], contract, preferred_element_type=F32
    ) + lax.dot_general(db, w_ref[1], contract, preferred_element_type=F32)
    pc_ref[...] += jnp.sum(h * back, axis=1, keepdims=True)

    @pl.when(step == pl.num_programs(0) - 1)
    def _():
        pairs = px_ref.shape[0] // PACK
        half = px_ref.shape[1] // 2
        low = px_ref[:, :half]
        high = px_ref[:, half:]
        many = px_ref.shape[0]
        upper = iota((many, half), 0) % PACK < CAP
        low_up = pltpu.roll(low, many - CAP, 0)
        high_down = pltpu.roll(high, CAP, 0)
        even = jnp.where(upper, low, high_down)
        odd = jnp.where(upper, low_up, high)
        pc = pc_ref[...]
        pc_up = pltpu.roll(pc, many - CAP, 0)
        for q in range(pairs):
            at = slice(q * PACK, (q + 1) * PACK)
            back_ref[2 * q, :, :half] = even[at].astype(BF)
            back_ref[2 * q, :, half:] = pc[at].astype(BF)
            back_ref[2 * q + 1, :, :half] = odd[at].astype(BF)
            back_ref[2 * q + 1, :, half:] = pc_up[at].astype(BF)


def weight_kernel(order_ref, cols_ref, *refs):
    hid_refs, out_ref, left_ref = refs[:-2], refs[-2], refs[-1]
    members = len(hid_refs)
    many = hid_refs[0].shape[1]

    @pl.when(pl.program_id(0) == 0)
    def _():
        sources = many // CAP
        block = 8 if sources % 8 == 0 else sources
        rows = block * CAP
        row, col = iota((rows, block * PACK), 0), iota((rows, block * PACK), 1)
        source = row // CAP * PACK + row % CAP
        take = [(col == source + k * CAP).astype(BF) for k in range(2)]
        for m in range(members):
            for at in range(sources // block):
                start = order_ref[m] * (sources * PACK) + at * block * PACK
                piece = cols_ref[pl.ds(pl.multiple_of(start, PACK), block * PACK), :]
                for k in range(2):
                    left_ref[k, pl.ds(m * many + at * rows, rows), :] = jnp.dot(
                        take[k], piece, preferred_element_type=F32
                    ).astype(BF)

    contract = (((0,), (0,)), ((), ()))
    for k in range(3):
        right = jnp.concatenate([ref[k] for ref in hid_refs], axis=0)
        out_ref[k] = lax.dot_general(
            left_ref[k // 2], right, contract, preferred_element_type=F32
        )


def token_kernel(ids_ref, recv_ref, tok_ref, comb_ref, *, grp_size):
    ids = ids_ref[...]
    both = slots(ids)
    peers = recv_ref.shape[0]
    tokens = ids.shape[1]
    half = tok_ref.shape[1] // (2 * grp_size)
    upper = iota((PACK, tokens), 0) < CAP
    contract = (((0,), (0,)), ((), ()))
    picks = [
        jnp.where(upper, both, 0.0).astype(BF),
        jnp.where(upper, 0.0, both).astype(BF),
    ]
    for side in range(grp_size):
        total = recv_ref[side].astype(F32)
        for at in range(side + grp_size, peers, grp_size):
            total = total + recv_ref[at].astype(F32)
        if side == 0:
            pc = total[:, half:]
            per = jnp.sum(
                jnp.where(upper, both, 0.0) * pc[:, :1], axis=0, keepdims=True
            )
            comb_ref[...] = jnp.where(ids == 0, per, 0.0)
        rounded = total[:, :half].astype(BF)
        for part in range(2):
            start = (2 * side + part) * half
            tok_ref[:, start : start + half] = lax.dot_general(
                picks[part], rounded, contract, preferred_element_type=F32
            ).astype(BF)


def local(tokens, grad_out, expert_ids, combine, weights):
    ep_size = lax.axis_size("ep")
    rep_size = lax.axis_size("rep")
    grp_size = lax.axis_size("grp")
    token_count, model_width = tokens.shape
    peers = ep_size * grp_size
    many = peers * CAP
    depth, _, hidden = weights.shape
    owners = rep_size * grp_size
    owner_rows = model_width // owners
    side_width = depth + LANES
    vmem = pl.BlockSpec(memory_space=pltpu.VMEM)
    ids = expert_ids.T
    w = jnp.transpose(weights, (1, 0, 2))

    rows, cols = pl.pallas_call(
        functools.partial(pack_kernel, grp_size=grp_size, owners=owners),
        out_shape=(
            jax.ShapeDtypeStruct((peers, PACK, side_width), BF),
            jax.ShapeDtypeStruct((rep_size * peers, PACK, owner_rows), BF),
        ),
        in_specs=[vmem] * 4,
        out_specs=(vmem, vmem),
        name="pack",
    )(ids, combine.T, tokens, grad_out)

    recv = lax.all_to_all(rows, ("ep", "grp"), 0, 0, tiled=True)
    recv = recv.reshape(peers * PACK, side_width)
    col_recv = lax.all_to_all(cols, ("rep", "ep", "grp"), 0, 0, tiled=True)
    col_recv = col_recv.reshape(rep_size * peers * PACK, owner_rows)

    tile = tile_of(hidden, 256)
    steps = hidden // tile
    own, send, scale = pl.pallas_call(
        forward_kernel,
        grid=(steps,),
        out_shape=(
            jax.ShapeDtypeStruct((3, many, hidden), F32),
            jax.ShapeDtypeStruct((3, many, hidden), BF),
            jax.ShapeDtypeStruct((many, LANES), F32),
        ),
        in_specs=[
            pl.BlockSpec((peers * PACK, side_width), lambda i: (0, 0)),
            pl.BlockSpec((3, depth, tile), lambda i: (0, 0, i)),
        ],
        out_specs=(
            pl.BlockSpec((3, many, tile), lambda i: (0, 0, i)),
            pl.BlockSpec((3, many, tile), lambda i: (0, 0, i)),
            pl.BlockSpec((many, LANES), lambda i: (0, 0)),
        ),
        scratch_shapes=[pltpu.VMEM((2, many, depth), BF)],
        name="forward",
    )(recv, w)

    if grp_size == 2:
        other = lax.ppermute(send, "grp", [(0, 1), (1, 0)])
    else:
        other = (lax.psum(send.astype(F32), "grp") - send.astype(F32)).astype(BF)

    hid, back = pl.pallas_call(
        hidden_kernel,
        grid=(steps,),
        out_shape=(
            jax.ShapeDtypeStruct((3, many, hidden), BF),
            jax.ShapeDtypeStruct((peers, PACK, depth // 2 + LANES), BF),
        ),
        in_specs=[
            pl.BlockSpec((3, many, tile), lambda i: (0, 0, i)),
            pl.BlockSpec((3, many, tile), lambda i: (0, 0, i)),
            pl.BlockSpec((many, LANES), lambda i: (0, 0)),
            pl.BlockSpec((2, depth, tile), lambda i: (0, 0, i)),
        ],
        out_specs=(
            pl.BlockSpec((3, many, tile), lambda i: (0, 0, i)),
            pl.BlockSpec((peers, PACK, depth // 2 + LANES), lambda i: (0, 0, 0)),
        ),
        scratch_shapes=[
            pltpu.VMEM((many, depth), F32),
            pltpu.VMEM((many, LANES), F32),
        ],
        name="hidden",
    )(own, other, scale, w)

    back_recv = lax.all_to_all(back, ("ep", "grp"), 0, 0, tiled=True)

    gathered = [hid]
    flips = [0]
    step = rep_size // 2
    while step:
        pairs = [(i, i ^ step) for i in range(rep_size)]
        gathered += [lax.ppermute(piece, "rep", pairs) for piece in gathered]
        flips += [flip ^ step for flip in flips]
        step //= 2
    order = jnp.bitwise_xor(lax.axis_index("rep"), jnp.array(flips, jnp.int32))

    grad_weights = pl.pallas_call(
        weight_kernel,
        grid=(steps,),
        out_shape=jax.ShapeDtypeStruct((3, owner_rows, hidden), F32),
        in_specs=[
            pl.BlockSpec(memory_space=pltpu.SMEM),
            pl.BlockSpec((rep_size * peers * PACK, owner_rows), lambda i: (0, 0)),
        ]
        + [pl.BlockSpec((3, many, tile), lambda i: (0, 0, i))] * rep_size,
        out_specs=pl.BlockSpec((3, owner_rows, tile), lambda i: (0, 0, i)),
        scratch_shapes=[pltpu.VMEM((2, rep_size * many, owner_rows), BF)],
        name="weight",
    )(order, col_recv, *gathered)

    grad_tokens, grad_combine = pl.pallas_call(
        functools.partial(token_kernel, grp_size=grp_size),
        out_shape=(
            jax.ShapeDtypeStruct((token_count, model_width), BF),
            jax.ShapeDtypeStruct((2, token_count), F32),
        ),
        in_specs=[vmem] * 2,
        out_specs=(vmem, vmem),
        name="token",
    )(ids, back_recv)

    return (grad_tokens, grad_combine.T, jnp.transpose(grad_weights, (1, 0, 2)))


def solution(mesh):
    in_specs = (
        P(("rep", "ep", "grp"), None),
        P(("rep", "ep", "grp"), None),
        P(("rep", "ep", "grp"), None),
        P(("rep", "ep", "grp"), None),
        P("grp", None, "ep"),
    )
    out_specs = (
        P(("rep", "ep", "grp"), None),
        P(("rep", "ep", "grp"), None),
        P(("rep", "grp"), None, "ep"),
    )
    return jax.shard_map(local, mesh=mesh, in_specs=in_specs, out_specs=out_specs, check_vma=False)
```

```python
import functools

import jax
import jax.numpy as jnp
from jax import lax
from jax.experimental import pallas as pl
from jax.experimental.pallas import tpu as pltpu
from jax.sharding import PartitionSpec as P


CAP = 4
PACK = 2 * CAP
LANES = 128
GRANT = 16 << 20
WHOLE = 60 * 1024 * 1024
BF = jnp.bfloat16
F32 = jnp.float32


def tile_of(extent, most):
    for tile in range(most, 0, -LANES):
        if tile % LANES == 0 and extent % tile == 0:
            return tile
    return extent


def cost(flops):
    return pl.CostEstimate(flops=flops, bytes_accessed=0, transcendentals=0)


def iota(shape, axis):
    return lax.broadcasted_iota(jnp.int32, shape, axis)


def slots(ids):
    tokens = ids.shape[1]
    named = jnp.sum((ids == 0).astype(F32), axis=0, keepdims=True)
    earlier = (iota((tokens, tokens), 0) < iota((tokens, tokens), 1)).astype(BF)
    wide = jnp.broadcast_to(named, (PACK, tokens))
    before = jnp.dot(wide.astype(BF), earlier, preferred_element_type=F32)
    slot = (iota((PACK, tokens), 0) % CAP).astype(F32)
    return jnp.where(before == slot, wide, 0.0)


def pack_kernel(*refs, grp_size, owners):
    sources, rows_ref = refs[:4], refs[4]
    held, done = refs[5:9], refs[9]
    loads = [
        pltpu.make_async_copy(source, target, done.at[n])
        for n, (source, target) in enumerate(zip(sources, held))
    ]
    for load in loads:
        load.start()
    for load in loads:
        load.wait()
    ids_ref, comb_ref, tok_ref, out_ref = held
    ids = ids_ref[...]
    both = slots(ids)
    model_width = tok_ref.shape[1]
    tokens = ids.shape[1]
    half = model_width // grp_size
    upper = iota((PACK, tokens), 0) < CAP
    first = jnp.where(upper, both, 0.0).astype(BF)
    second = jnp.where(upper, 0.0, both).astype(BF)
    packed = (
        jnp.dot(first, tok_ref[...], preferred_element_type=F32)
        + jnp.dot(second, out_ref[...], preferred_element_type=F32)
    ).astype(BF)
    chosen = jnp.sum(
        jnp.where(ids == 0, comb_ref[...].astype(F32), 0.0), axis=0, keepdims=True
    )
    scale = jnp.sum(both * chosen, axis=1, keepdims=True)
    scale = jnp.broadcast_to(scale, (PACK, LANES)).astype(BF)
    width = model_width // owners
    for peer in range(rows_ref.shape[0]):
        side = peer % grp_size
        rows_ref[peer, :, :half] = packed[:, side * half : (side + 1) * half]
        rows_ref[peer, :, half : half + LANES] = scale
        for rep in range(owners // grp_size):
            to = half + LANES + rep * width
            start = (rep * grp_size + side) * width
            rows_ref[peer, :, to : to + width] = packed[:, start : start + width]


def forward_kernel(
    recv_ref, far_ref, own_ref, send_ref, scale_ref, cols_ref, near_ref, down_ref, rows_ref, done, *, tile
):
    depth, hidden = far_ref.shape[1:]
    starts = range(0, hidden, tile)
    loads = []
    for n, start in enumerate(starts):
        here = pl.ds(start, tile)
        for k in range(3):
            loads.append(
                pltpu.make_async_copy(
                    far_ref.at[k, :, here],
                    down_ref.at[:, here] if k == 2 else near_ref.at[k, :, here],
                    done.at[3 * n + k],
                )
            )
    for load in loads:
        load.start()
    peers = recv_ref.shape[0] // PACK
    block = 8 if peers % 8 == 0 else peers
    many = block * CAP
    row, col = iota((many, block * PACK), 0), iota((many, block * PACK), 1)
    source = row // CAP * PACK + row % CAP
    take_x = (col == source).astype(BF)
    take_y = (col == source + CAP).astype(BF)
    for at in range(peers // block):
        piece = recv_ref[at * block * PACK : (at + 1) * block * PACK, : depth + LANES]
        xr = jnp.dot(take_x, piece, preferred_element_type=F32)
        yr = jnp.dot(take_y, piece[:, :depth], preferred_element_type=F32)
        here = pl.ds(at * many, many)
        rows_ref[0, here, :] = xr[:, :depth].astype(BF)
        rows_ref[1, here, :] = yr.astype(BF)
        scale_ref[here, :] = xr[:, depth:]
    cols_ref[...] = recv_ref[:, depth + LANES :]
    for n, start in enumerate(starts):
        here = slice(start, start + tile)
        for k in range(3):
            loads[3 * n + k].wait()
            right = down_ref[:, here] if k == 2 else near_ref[k, :, here]
            part = jnp.dot(rows_ref[k // 2], right, preferred_element_type=F32)
            own_ref[k, :, here] = part
            send_ref[k, :, here] = part.astype(BF)


def hidden_kernel(own_ref, other_ref, scale_ref, hid_ref, pc_ref, *, tile):
    cr = scale_ref[:, :1]
    pc = jnp.zeros((scale_ref.shape[0], 1), F32)
    for start in range(0, own_ref.shape[2], tile):
        here = slice(start, start + tile)
        a = own_ref[0, :, here] + other_ref[0, :, here].astype(F32)
        b = own_ref[1, :, here] + other_ref[1, :, here].astype(F32)
        back = own_ref[2, :, here] + other_ref[2, :, here].astype(F32)
        sig = jax.nn.sigmoid(a)
        act = a * sig
        h = act * b
        dh = cr * back
        hid_ref[0, :, here] = (dh * b * sig * (1.0 + a * (1.0 - sig))).astype(BF)
        hid_ref[1, :, here] = (dh * act).astype(BF)
        hid_ref[2, :, here] = (cr * h).astype(BF)
        pc = pc + jnp.sum(h * back, axis=1, keepdims=True)
    pc_ref[...] = jnp.broadcast_to(pc, pc_ref.shape)


def return_kernel(hid_ref, pc_ref, w_ref, back_ref):
    pc = pc_ref[...]
    contract = (((1,), (1,)), ((), ()))
    px = lax.dot_general(
        hid_ref[0], w_ref[0], contract, preferred_element_type=F32
    ) + lax.dot_general(hid_ref[1], w_ref[1], contract, preferred_element_type=F32)
    many = px.shape[0]
    half = px.shape[1] // 2
    low, high = px[:, :half], px[:, half:]
    upper = iota((many, half), 0) % PACK < CAP
    even = jnp.where(upper, low, pltpu.roll(high, CAP, 0))
    odd = jnp.where(upper, pltpu.roll(low, many - CAP, 0), high)
    pc_up = pltpu.roll(pc, many - CAP, 0)
    for q in range(many // PACK):
        at = slice(q * PACK, (q + 1) * PACK)
        back_ref[2 * q, :, :half] = even[at].astype(BF)
        back_ref[2 * q, :, half:] = pc[at].astype(BF)
        back_ref[2 * q + 1, :, :half] = odd[at].astype(BF)
        back_ref[2 * q + 1, :, half:] = pc_up[at].astype(BF)


def turn_kernel(rank_ref, *refs, many):
    cols_refs, (turned_ref, left_ref) = refs[:-2], refs[-2:]
    width = left_ref.shape[2]
    sources = many // CAP
    block = 8 if sources % 8 == 0 else sources
    rows = block * CAP
    row, col = iota((rows, block * PACK), 0), iota((rows, block * PACK), 1)
    source = row // CAP * PACK + row % CAP
    take = [(col == source + k * CAP).astype(BF) for k in range(2)]
    for m, cols_ref in enumerate(cols_refs):
        for at in range(sources // block):
            here = slice(at * block * PACK, (at + 1) * block * PACK)
            piece = cols_ref[here, :width]
            for rep in range(1, cols_ref.shape[1] // width):
                other = cols_ref[here, rep * width : (rep + 1) * width]
                piece = jnp.where(rank_ref[0] == rep, other, piece)
            for k in range(2):
                left_ref[k, pl.ds(m * many + at * rows, rows), :] = jnp.dot(
                    take[k], piece, preferred_element_type=F32
                )
    for k in range(2):
        turned_ref[k] = jnp.transpose(left_ref[k]).astype(BF)


def weight_kernel(turned_ref, *refs, tile):
    hid_refs, (out_ref, made_ref, done) = refs[:-3], refs[-3:]
    tiles = [
        (k, start) for start in range(0, hid_refs[0].shape[2], tile) for k in range(3)
    ]
    copies = [
        pltpu.make_async_copy(
            made_ref.at[k, :, pl.ds(start, tile)],
            out_ref.at[k, :, pl.ds(start, tile)],
            done.at[n],
        )
        for n, (k, start) in enumerate(tiles)
    ]
    for n, (k, start) in enumerate(tiles):
        here = slice(start, start + tile)
        right = jnp.concatenate([ref[k, :, here] for ref in hid_refs], axis=0)
        made_ref[k, :, here] = jnp.dot(
            turned_ref[k // 2], right, preferred_element_type=F32
        )
        if n:
            copies[n - 1].start()
    copies[-1].start()
    for copy in copies:
        copy.wait()


def token_kernel(ids_ref, recv_ref, tok_ref, comb_ref, *, grp_size):
    ids = ids_ref[...]
    both = slots(ids)
    peers = recv_ref.shape[0]
    tokens = ids.shape[1]
    half = tok_ref.shape[1] // (2 * grp_size)
    upper = iota((PACK, tokens), 0) < CAP
    contract = (((0,), (0,)), ((), ()))
    picks = [
        jnp.where(upper, both, 0.0).astype(BF),
        jnp.where(upper, 0.0, both).astype(BF),
    ]
    for side in range(grp_size):
        total = recv_ref[side].astype(F32)
        for at in range(side + grp_size, peers, grp_size):
            total = total + recv_ref[at].astype(F32)
        if side == 0:
            pc = total[:, half:]
            per = jnp.sum(
                jnp.where(upper, both, 0.0) * pc[:, :1], axis=0, keepdims=True
            )
            comb_ref[...] = jnp.where(ids == 0, per, 0.0)
        rounded = total[:, :half].astype(BF)
        for part in range(2):
            start = (2 * side + part) * half
            tok_ref[:, start : start + half] = lax.dot_general(
                picks[part], rounded, contract, preferred_element_type=F32
            ).astype(BF)


def gather(piece, rep_size):
    pieces = [piece]
    step = rep_size // 2
    while step:
        pairs = [(i, i ^ step) for i in range(rep_size)]
        pieces += [lax.ppermute(held, "rep", pairs) for held in pieces]
        step //= 2
    return pieces


def local(tokens, grad_out, expert_ids, combine, weights):
    ep_size = lax.axis_size("ep")
    rep_size = lax.axis_size("rep")
    grp_size = lax.axis_size("grp")
    token_count, model_width = tokens.shape
    peers = ep_size * grp_size
    many = peers * CAP
    depth, _, hidden = weights.shape
    owners = rep_size * grp_size
    owner_rows = model_width // owners
    side_width = depth + LANES + rep_size * owner_rows
    vmem = pl.BlockSpec(memory_space=pltpu.VMEM)
    hbm = pl.BlockSpec(memory_space=pltpu.HBM)
    ids = expert_ids.T
    w = jnp.transpose(weights, (1, 0, 2))

    rank = lax.axis_index("rep").astype(jnp.int32).reshape(1)
    ids, rank = lax.optimization_barrier((ids, rank))
    rows = pl.pallas_call(
        functools.partial(pack_kernel, grp_size=grp_size, owners=owners),
        out_shape=jax.ShapeDtypeStruct((peers, PACK, side_width), BF),
        in_specs=[hbm] * 4,
        out_specs=vmem,
        scratch_shapes=[
            pltpu.VMEM(ids.shape, ids.dtype),
            pltpu.VMEM(ids.shape, combine.dtype),
            pltpu.VMEM(tokens.shape, tokens.dtype),
            pltpu.VMEM(grad_out.shape, grad_out.dtype),
            pltpu.SemaphoreType.DMA((4,)),
        ],
        compiler_params=pltpu.CompilerParams(vmem_limit_bytes=WHOLE),
        cost_estimate=cost(2_000_000_000),
        name="pack",
    )(ids, combine.T, tokens, grad_out)

    recv = lax.all_to_all(rows, ("ep", "grp"), 0, 0, tiled=True)
    recv = recv.reshape(peers * PACK, side_width)

    tile = tile_of(hidden, 256)
    own, send, scale, cols, near = pl.pallas_call(
        functools.partial(forward_kernel, tile=tile),
        out_shape=(
            jax.ShapeDtypeStruct((3, many, hidden), F32),
            jax.ShapeDtypeStruct((3, many, hidden), BF),
            jax.ShapeDtypeStruct((many, LANES), F32),
            jax.ShapeDtypeStruct((peers * PACK, rep_size * owner_rows), BF),
            jax.ShapeDtypeStruct((2, depth, hidden), BF),
        ),
        in_specs=[vmem, hbm],
        out_specs=(vmem,) * 5,
        scratch_shapes=[
            pltpu.VMEM((depth, hidden), BF),
            pltpu.VMEM((2, many, depth), BF),
            pltpu.SemaphoreType.DMA((3 * (hidden // tile),)),
        ],
        compiler_params=pltpu.CompilerParams(vmem_limit_bytes=WHOLE - (20 << 20)),
        cost_estimate=cost(3_000_000_000),
        name="forward",
    )(recv, w)

    gathered_cols = gather(cols, rep_size)
    turned = pl.pallas_call(
        functools.partial(turn_kernel, many=many),
        out_shape=jax.ShapeDtypeStruct((2, owner_rows, rep_size * many), BF),
        in_specs=[pl.BlockSpec(memory_space=pltpu.SMEM)] + [vmem] * rep_size,
        out_specs=vmem,
        scratch_shapes=[pltpu.VMEM((2, rep_size * many, owner_rows), F32)],
        compiler_params=pltpu.CompilerParams(vmem_limit_bytes=GRANT),
        cost_estimate=cost(1_000_000_000),
        name="turn",
    )(rank, *gathered_cols)

    if grp_size == 2:
        other = lax.ppermute(send, "grp", [(0, 1), (1, 0)])
    else:
        other = (lax.psum(send.astype(F32), "grp") - send.astype(F32)).astype(BF)

    other, turned = lax.optimization_barrier((other, turned))

    hid, pc = pl.pallas_call(
        functools.partial(hidden_kernel, tile=tile),
        out_shape=(
            jax.ShapeDtypeStruct((3, many, hidden), BF),
            jax.ShapeDtypeStruct((many, LANES), F32),
        ),
        in_specs=[vmem] * 3,
        out_specs=(vmem,) * 2,
        compiler_params=pltpu.CompilerParams(vmem_limit_bytes=GRANT),
        cost_estimate=cost(1_000_000_000),
        name="hidden",
    )(own, other, scale)

    back = pl.pallas_call(
        return_kernel,
        out_shape=jax.ShapeDtypeStruct((peers, PACK, depth // 2 + LANES), BF),
        in_specs=[vmem] * 3,
        out_specs=vmem,
        compiler_params=pltpu.CompilerParams(vmem_limit_bytes=GRANT),
        cost_estimate=cost(3_000_000_000),
        name="back",
    )(hid, pc, near)

    back_recv = lax.all_to_all(back, ("ep", "grp"), 0, 0, tiled=True)

    gathered = gather(hid, rep_size)
    grad_weights = pl.pallas_call(
        functools.partial(weight_kernel, tile=tile),
        out_shape=jax.ShapeDtypeStruct((3, owner_rows, hidden), F32),
        in_specs=[vmem] * (1 + rep_size),
        out_specs=pl.BlockSpec(memory_space=pl.ANY),
        scratch_shapes=[
            pltpu.VMEM((3, owner_rows, hidden), F32),
            pltpu.SemaphoreType.DMA((3 * (hidden // tile),)),
        ],
        compiler_params=pltpu.CompilerParams(vmem_limit_bytes=GRANT),
        cost_estimate=cost(6_000_000_000),
        name="weight",
    )(turned, *gathered)

    grad_tokens, grad_combine = pl.pallas_call(
        functools.partial(token_kernel, grp_size=grp_size),
        out_shape=(
            jax.ShapeDtypeStruct((token_count, model_width), BF),
            jax.ShapeDtypeStruct((2, token_count), F32),
        ),
        in_specs=[vmem] * 2,
        out_specs=(vmem, vmem),
        compiler_params=pltpu.CompilerParams(vmem_limit_bytes=GRANT),
        cost_estimate=cost(2_000_000_000),
        name="token",
    )(ids, back_recv)

    return (grad_tokens, grad_combine.T, jnp.transpose(grad_weights, (1, 0, 2)))


def solution(mesh):
    in_specs = (
        P(("rep", "ep", "grp"), None),
        P(("rep", "ep", "grp"), None),
        P(("rep", "ep", "grp"), None),
        P(("rep", "ep", "grp"), None),
        P("grp", None, "ep"),
    )
    out_specs = (
        P(("rep", "ep", "grp"), None),
        P(("rep", "ep", "grp"), None),
        P(("rep", "grp"), None, "ep"),
    )
    return jax.shard_map(
        local, mesh=mesh, in_specs=in_specs, out_specs=out_specs, check_vma=False
    )
```

```python
import functools

import jax
import jax.numpy as jnp
from jax import lax
from jax.experimental import pallas as pl
from jax.experimental.pallas import tpu as pltpu
from jax.sharding import PartitionSpec as P


CAP = 4
PACK = 2 * CAP
LANES = 128
GRANT = 16 << 20
WHOLE = 60 * 1024 * 1024
BF = jnp.bfloat16
F32 = jnp.float32


def tile_of(extent, most):
    for tile in range(most, 0, -LANES):
        if tile % LANES == 0 and extent % tile == 0:
            return tile
    return extent


def cost(flops):
    return pl.CostEstimate(flops=flops, bytes_accessed=0, transcendentals=0)


def iota(shape, axis):
    return lax.broadcasted_iota(jnp.int32, shape, axis)


def slots(ids):
    tokens = ids.shape[1]
    named = jnp.sum((ids == 0).astype(F32), axis=0, keepdims=True)
    earlier = (iota((tokens, tokens), 0) < iota((tokens, tokens), 1)).astype(BF)
    wide = jnp.broadcast_to(named, (PACK, tokens))
    before = jnp.dot(wide.astype(BF), earlier, preferred_element_type=F32)
    slot = (iota((PACK, tokens), 0) % CAP).astype(F32)
    return jnp.where(before == slot, wide, 0.0)


def pack_kernel(*refs, grp_size, owners):
    sources, rows_ref = refs[:4], refs[4]
    held, done = refs[5:9], refs[9]
    loads = [
        pltpu.make_async_copy(source, target, done.at[n])
        for n, (source, target) in enumerate(zip(sources, held))
    ]
    for load in loads:
        load.start()
    for load in loads:
        load.wait()
    ids_ref, comb_ref, tok_ref, out_ref = held
    ids = ids_ref[...]
    both = slots(ids)
    model_width = tok_ref.shape[1]
    tokens = ids.shape[1]
    half = model_width // grp_size
    upper = iota((PACK, tokens), 0) < CAP
    first = jnp.where(upper, both, 0.0).astype(BF)
    second = jnp.where(upper, 0.0, both).astype(BF)
    packed = (
        jnp.dot(first, tok_ref[...], preferred_element_type=F32)
        + jnp.dot(second, out_ref[...], preferred_element_type=F32)
    ).astype(BF)
    chosen = jnp.sum(
        jnp.where(ids == 0, comb_ref[...].astype(F32), 0.0), axis=0, keepdims=True
    )
    scale = jnp.sum(both * chosen, axis=1, keepdims=True)
    scale = jnp.broadcast_to(scale, (PACK, LANES)).astype(BF)
    width = model_width // owners
    for peer in range(rows_ref.shape[0]):
        side = peer % grp_size
        rows_ref[peer, :, :half] = packed[:, side * half : (side + 1) * half]
        rows_ref[peer, :, half : half + LANES] = scale
        for rep in range(owners // grp_size if rows_ref.shape[2] > half + LANES else 0):
            to = half + LANES + rep * width
            start = (rep * grp_size + side) * width
            rows_ref[peer, :, to : to + width] = packed[:, start : start + width]


def select_rows(recv_ref, first, depth, pick):
    peers = recv_ref.shape[0] // PACK
    block = 8 if peers % 8 == 0 else peers
    many = block * CAP
    row, col = iota((many, block * PACK), 0), iota((many, block * PACK), 1)
    take = (col == row // CAP * PACK + row % CAP + pick * CAP).astype(BF)
    for at in range(peers // block):
        piece = recv_ref[at * block * PACK : (at + 1) * block * PACK, first : first + depth]
        yield pl.ds(at * many, many), jnp.dot(take, piece, preferred_element_type=F32)


def forward_kernel(recv_ref, far_ref, *refs, cuts):
    own_ref, scale_ref, near_ref = refs[:3]
    send_refs = refs[3 : 3 + len(cuts)]
    cols_refs, (down_ref, rows_ref, done) = refs[3 + len(cuts) : -3], refs[-3:]
    depth = far_ref.shape[1]
    piece = tile_of(depth, 256)
    pieces = [slice(at, at + piece) for at in range(0, depth, piece)]
    loads = []
    for n, here in enumerate(pieces):
        for k in range(3):
            target = down_ref if k == 2 else near_ref.at[k]
            loads.append(
                pltpu.make_async_copy(
                    far_ref.at[k, here], target.at[here], done.at[3 * n + k]
                )
            )
    for load in loads:
        load.start()
    for here, xr in select_rows(recv_ref, 0, depth + LANES, 0):
        rows_ref[0, here, :] = xr[:, :depth].astype(BF)
        scale_ref[here, :] = xr[:, depth:]
    for here, yr in select_rows(recv_ref, 0, depth, 1):
        rows_ref[1, here, :] = yr.astype(BF)
    for cols_ref in cols_refs:
        cols_ref[...] = recv_ref[:, depth + LANES :]
    for n, here in enumerate(pieces):
        last = n == len(pieces) - 1
        for k in range(3):
            loads[3 * n + k].wait()
            right_ref = down_ref if k == 2 else near_ref.at[k]
            for cut, send_ref in zip(cuts, send_refs):
                part = jnp.dot(
                    rows_ref[k // 2, :, here], right_ref[here, cut], preferred_element_type=F32
                )
                if n:
                    part = part + own_ref[k, :, cut]
                own_ref[k, :, cut] = part
                if last:
                    send_ref[k] = part.astype(BF)


def hidden_kernel(own_ref, other_ref, scale_ref, hid_ref, pc_ref, *, cut, tile):
    cr = scale_ref[:, :1]
    pc = jnp.zeros((scale_ref.shape[0], 1), F32)
    for start in range(0, hid_ref.shape[2], tile):
        here = slice(start, start + tile)
        mine = slice(cut.start + start, cut.start + start + tile)
        a = own_ref[0, :, mine] + other_ref[0, :, here].astype(F32)
        b = own_ref[1, :, mine] + other_ref[1, :, here].astype(F32)
        back = own_ref[2, :, mine] + other_ref[2, :, here].astype(F32)
        sig = jax.nn.sigmoid(a)
        act = a * sig
        h = act * b
        dh = cr * back
        hid_ref[0, :, here] = (dh * b * sig * (1.0 + a * (1.0 - sig))).astype(BF)
        hid_ref[1, :, here] = (dh * act).astype(BF)
        hid_ref[2, :, here] = (cr * h).astype(BF)
        pc = pc + jnp.sum(h * back, axis=1, keepdims=True)
    pc_ref[...] = jnp.broadcast_to(pc, pc_ref.shape)


def return_kernel(hid_ref, pc_ref, near_ref, *refs, cut, last):
    contract = (((1,), (1,)), ((), ()))
    px = lax.dot_general(
        hid_ref[0], near_ref[0, :, cut], contract, preferred_element_type=F32
    ) + lax.dot_general(hid_ref[1], near_ref[1, :, cut], contract, preferred_element_type=F32)
    pc = pc_ref[...]
    if cut.start:
        px = px + refs[0][...]
        pc = pc + refs[1][...]
    if not last:
        refs[-2][...] = px
        refs[-1][...] = pc
        return
    back_ref = refs[-1]
    many = px.shape[0]
    half = px.shape[1] // 2
    low, high = px[:, :half], px[:, half:]
    upper = iota((many, half), 0) % PACK < CAP
    even = jnp.where(upper, low, pltpu.roll(high, CAP, 0))
    odd = jnp.where(upper, pltpu.roll(low, many - CAP, 0), high)
    pc_up = pltpu.roll(pc, many - CAP, 0)
    for q in range(many // PACK):
        at = slice(q * PACK, (q + 1) * PACK)
        back_ref[2 * q, :, :half] = even[at].astype(BF)
        back_ref[2 * q, :, half:] = pc[at].astype(BF)
        back_ref[2 * q + 1, :, :half] = odd[at].astype(BF)
        back_ref[2 * q + 1, :, half:] = pc_up[at].astype(BF)


def split_kernel(rep_ref, grp_ref, near_ref, far_ref, keep_ref, give_ref, *, width):
    blocks = keep_ref.shape[1] // width
    rep_high, grp = rep_ref[0] // blocks, grp_ref[0]

    def owned(ref, at, side):
        start = (2 * at + side) * width
        return ref[:, start : start + width]

    for at in range(blocks):
        mine = jnp.where(grp == 0, owned(near_ref, at, 0), owned(near_ref, at, 1))
        theirs = jnp.where(grp == 0, owned(far_ref, at, 0), owned(far_ref, at, 1))
        here = slice(at * width, (at + 1) * width)
        keep_ref[:, here] = jnp.where(rep_high == grp, mine, theirs)
        give_ref[:, here] = jnp.where(rep_high == grp, theirs, mine)


def turn_kernel(rank_ref, *refs, many):
    cols_refs, (turned_ref, left_ref) = refs[:-2], refs[-2:]
    width = left_ref.shape[2]
    sources = many // CAP
    block = 8 if sources % 8 == 0 else sources
    rows = block * CAP
    row, col = iota((rows, block * PACK), 0), iota((rows, block * PACK), 1)
    source = row // CAP * PACK + row % CAP
    take = [(col == source + k * CAP).astype(BF) for k in range(2)]
    for m, cols_ref in enumerate(cols_refs):
        for at in range(sources // block):
            here = slice(at * block * PACK, (at + 1) * block * PACK)
            piece = cols_ref[here, :width]
            blocks = cols_ref.shape[1] // width
            for rep in range(1, blocks):
                other = cols_ref[here, rep * width : (rep + 1) * width]
                piece = jnp.where(rank_ref[0] % blocks == rep, other, piece)
            for k in range(2):
                left_ref[k, pl.ds(m * many + at * rows, rows), :] = jnp.dot(
                    take[k], piece, preferred_element_type=F32
                )
    for k in range(2):
        turned_ref[k] = jnp.transpose(left_ref[k]).astype(BF)


def weight_kernel(turned_ref, *refs, cuts, tile):
    hid_refs, (out_ref, made_ref, done) = refs[:-3], refs[-3:]
    members = len(hid_refs) // len(cuts)
    tiles = []
    for c, cut in enumerate(cuts):
        pieces = hid_refs[c * members : (c + 1) * members]
        for start in range(0, cut.stop - cut.start, tile):
            tiles += [(k, cut.start + start, start, pieces) for k in range(3)]
    copies = [
        pltpu.make_async_copy(
            made_ref.at[k, :, pl.ds(to, tile)], out_ref.at[k, :, pl.ds(to, tile)], done.at[n]
        )
        for n, (k, to, _, _) in enumerate(tiles)
    ]
    for n, (k, to, start, pieces) in enumerate(tiles):
        here = slice(start, start + tile)
        right = jnp.concatenate([ref[k, :, here] for ref in pieces], axis=0)
        made_ref[k, :, to : to + tile] = jnp.dot(
            turned_ref[k // 2], right, preferred_element_type=F32
        )
        if n:
            copies[n - 1].start()
    copies[-1].start()
    for copy in copies:
        copy.wait()


def token_kernel(ids_ref, recv_ref, tok_ref, comb_ref, *, grp_size):
    ids = ids_ref[...]
    both = slots(ids)
    peers = recv_ref.shape[0]
    tokens = ids.shape[1]
    half = tok_ref.shape[1] // (2 * grp_size)
    upper = iota((PACK, tokens), 0) < CAP
    contract = (((0,), (0,)), ((), ()))
    picks = [
        jnp.where(upper, both, 0.0).astype(BF),
        jnp.where(upper, 0.0, both).astype(BF),
    ]
    for side in range(grp_size):
        total = recv_ref[side].astype(F32)
        for at in range(side + grp_size, peers, grp_size):
            total = total + recv_ref[at].astype(F32)
        if side == 0:
            pc = total[:, half:]
            per = jnp.sum(
                jnp.where(upper, both, 0.0) * pc[:, :1], axis=0, keepdims=True
            )
            comb_ref[...] = jnp.where(ids == 0, per, 0.0)
        rounded = total[:, :half].astype(BF)
        for part in range(2):
            start = (2 * side + part) * half
            tok_ref[:, start : start + half] = lax.dot_general(
                picks[part], rounded, contract, preferred_element_type=F32
            ).astype(BF)


def gather(piece, rep_size, give=None):
    pieces = [piece]
    step = rep_size // 2
    while step:
        pairs = [(i, i ^ step) for i in range(rep_size)]
        sent = [give] if give is not None and len(pieces) == 1 else pieces
        pieces = pieces + [lax.ppermute(held, "rep", pairs) for held in sent]
        step //= 2
    return pieces


def local(tokens, grad_out, expert_ids, combine, weights):
    ep_size = lax.axis_size("ep")
    rep_size = lax.axis_size("rep")
    grp_size = lax.axis_size("grp")
    token_count, model_width = tokens.shape
    peers = ep_size * grp_size
    many = peers * CAP
    depth, _, hidden = weights.shape
    owners = rep_size * grp_size
    owner_rows = model_width // owners
    paired = grp_size == 2 and rep_size % 4 == 0
    side_width = depth + LANES + (0 if paired else rep_size * owner_rows)
    vmem = pl.BlockSpec(memory_space=pltpu.VMEM)
    hbm = pl.BlockSpec(memory_space=pltpu.HBM)
    ids = expert_ids.T
    w = jnp.transpose(weights, (1, 0, 2))

    rep = lax.axis_index("rep").astype(jnp.int32).reshape(1)
    grp = lax.axis_index("grp").astype(jnp.int32).reshape(1)
    ids, rep, grp = lax.optimization_barrier((ids, rep, grp))
    rows = pl.pallas_call(
        functools.partial(pack_kernel, grp_size=grp_size, owners=owners),
        out_shape=jax.ShapeDtypeStruct((peers, PACK, side_width), BF),
        in_specs=[hbm] * 4,
        out_specs=vmem,
        scratch_shapes=[
            pltpu.VMEM(ids.shape, ids.dtype),
            pltpu.VMEM(ids.shape, combine.dtype),
            pltpu.VMEM(tokens.shape, tokens.dtype),
            pltpu.VMEM(grad_out.shape, grad_out.dtype),
            pltpu.SemaphoreType.DMA((4,)),
        ],
        compiler_params=pltpu.CompilerParams(vmem_limit_bytes=WHOLE),
        cost_estimate=cost(2_000_000_000),
        name="pack",
    )(ids, combine.T, tokens, grad_out)

    recv = lax.all_to_all(rows, ("ep", "grp"), 0, 0, tiled=True)
    recv = recv.reshape(peers * PACK, side_width)

    if paired:
        far_recv = lax.ppermute(recv, "grp", [(0, 1), (1, 0)])

    tile = tile_of(hidden, 256)
    middle = -(-hidden // (2 * tile)) * tile
    cuts = [slice(0, hidden)]
    if middle < hidden:
        cuts = [slice(0, middle), slice(middle, hidden)]
    widths = [cut.stop - cut.start for cut in cuts]
    own, scale, near, *sends = pl.pallas_call(
        functools.partial(forward_kernel, cuts=cuts),
        out_shape=(
            jax.ShapeDtypeStruct((3, many, hidden), F32),
            jax.ShapeDtypeStruct((many, LANES), F32),
            jax.ShapeDtypeStruct((2, depth, hidden), BF),
            *(jax.ShapeDtypeStruct((3, many, width), BF) for width in widths),
            *(
                jax.ShapeDtypeStruct((peers * PACK, rep_size * owner_rows), BF)
                for _ in range(0 if paired else 1)
            ),
        ),
        in_specs=[vmem, hbm],
        out_specs=(vmem,) * (3 + len(cuts) + (0 if paired else 1)),
        scratch_shapes=[
            pltpu.VMEM((depth, hidden), BF),
            pltpu.VMEM((2, many, depth), BF),
            pltpu.SemaphoreType.DMA((3 * (depth // tile_of(depth, 256)),)),
        ],
        compiler_params=pltpu.CompilerParams(vmem_limit_bytes=WHOLE - (20 << 20)),
        cost_estimate=cost(3_000_000_000),
        name="forward",
    )(recv, w)

    others = []
    for c in range(len(cuts)):
        send = sends[c]
        if grp_size == 2:
            others.append(lax.ppermute(send, "grp", [(0, 1), (1, 0)]))
        else:
            total = lax.psum(send.astype(F32), "grp")
            others.append((total - send.astype(F32)).astype(BF))

    if paired:
        side = (rep_size // 2) * owner_rows
        keep, give = pl.pallas_call(
            functools.partial(split_kernel, width=owner_rows),
            out_shape=(jax.ShapeDtypeStruct((peers * PACK, side), BF),) * 2,
            in_specs=[pl.BlockSpec(memory_space=pltpu.SMEM)] * 2 + [vmem] * 2,
            out_specs=(vmem,) * 2,
            compiler_params=pltpu.CompilerParams(vmem_limit_bytes=GRANT),
            cost_estimate=cost(500_000_000),
            name="split",
        )(rep, grp, recv, far_recv)
        gathered_cols = gather(keep, rep_size, give)
    else:
        gathered_cols = gather(sends[-1], rep_size)
    turned = pl.pallas_call(
        functools.partial(turn_kernel, many=many),
        out_shape=jax.ShapeDtypeStruct((2, owner_rows, rep_size * many), BF),
        in_specs=[pl.BlockSpec(memory_space=pltpu.SMEM)] + [vmem] * rep_size,
        out_specs=vmem,
        scratch_shapes=[pltpu.VMEM((2, rep_size * many, owner_rows), F32)],
        compiler_params=pltpu.CompilerParams(vmem_limit_bytes=GRANT),
        cost_estimate=cost(500_000_000),
        name="turn",
    )(rep, *gathered_cols)
    others[-1], turned = lax.optimization_barrier((others[-1], turned))

    gathered = []
    back = []
    for c, cut in enumerate(cuts):
        last = c == len(cuts) - 1
        hid, pc = pl.pallas_call(
            functools.partial(hidden_kernel, cut=cut, tile=tile),
            out_shape=(
                jax.ShapeDtypeStruct((3, many, widths[c]), BF),
                jax.ShapeDtypeStruct((many, LANES), F32),
            ),
            in_specs=[vmem] * 3,
            out_specs=(vmem,) * 2,
            compiler_params=pltpu.CompilerParams(vmem_limit_bytes=GRANT),
            cost_estimate=cost(1_000_000_000),
        )(own, others[c], scale)
        if last:
            shapes = jax.ShapeDtypeStruct((peers, PACK, depth // 2 + LANES), BF)
        else:
            shapes = (
                jax.ShapeDtypeStruct((many, depth), F32),
                jax.ShapeDtypeStruct((many, LANES), F32),
            )
        back = pl.pallas_call(
            functools.partial(return_kernel, cut=cut, last=last),
            out_shape=shapes,
            in_specs=[vmem] * (3 + len(back)),
            out_specs=vmem if last else (vmem,) * 2,
            compiler_params=pltpu.CompilerParams(vmem_limit_bytes=GRANT),
            cost_estimate=cost(3_000_000_000),
        )(hid, pc, near, *back)
        gathered += gather(hid, rep_size)

    back_recv = lax.all_to_all(back, ("ep", "grp"), 0, 0, tiled=True)

    grad_weights = pl.pallas_call(
        functools.partial(weight_kernel, cuts=cuts, tile=tile),
        out_shape=jax.ShapeDtypeStruct((3, owner_rows, hidden), F32),
        in_specs=[vmem] * (1 + len(gathered)),
        out_specs=pl.BlockSpec(memory_space=pl.ANY),
        scratch_shapes=[
            pltpu.VMEM((3, owner_rows, hidden), F32),
            pltpu.SemaphoreType.DMA((3 * (hidden // tile),)),
        ],
        compiler_params=pltpu.CompilerParams(vmem_limit_bytes=GRANT),
        cost_estimate=cost(6_000_000_000),
        name="weight",
    )(turned, *gathered)

    grad_tokens, grad_combine = pl.pallas_call(
        functools.partial(token_kernel, grp_size=grp_size),
        out_shape=(
            jax.ShapeDtypeStruct((token_count, model_width), BF),
            jax.ShapeDtypeStruct((2, token_count), F32),
        ),
        in_specs=[vmem] * 2,
        out_specs=(vmem, vmem),
        compiler_params=pltpu.CompilerParams(vmem_limit_bytes=GRANT),
        cost_estimate=cost(2_000_000_000),
        name="token",
    )(ids, back_recv)

    return (grad_tokens, grad_combine.T, jnp.transpose(grad_weights, (1, 0, 2)))


def solution(mesh):
    in_specs = (
        P(("rep", "ep", "grp"), None),
        P(("rep", "ep", "grp"), None),
        P(("rep", "ep", "grp"), None),
        P(("rep", "ep", "grp"), None),
        P("grp", None, "ep"),
    )
    out_specs = (
        P(("rep", "ep", "grp"), None),
        P(("rep", "ep", "grp"), None),
        P(("rep", "grp"), None, "ep"),
    )
    return jax.shard_map(
        local, mesh=mesh, in_specs=in_specs, out_specs=out_specs, check_vma=False
    )
```

```python
import functools

import jax
import jax.numpy as jnp
from jax import lax
from jax.experimental import pallas as pl
from jax.experimental.pallas import tpu as pltpu
from jax.sharding import PartitionSpec as P


CAP = 4
PACK = 2 * CAP
LANES = 128
GRANT = 16 << 20
WHOLE = 60 * 1024 * 1024
BF = jnp.bfloat16
F32 = jnp.float32


def tile_of(extent, most):
    for tile in range(most, 0, -LANES):
        if tile % LANES == 0 and extent % tile == 0:
            return tile
    return extent


def cost(flops):
    return pl.CostEstimate(flops=flops, bytes_accessed=0, transcendentals=0)


def iota(shape, axis):
    return lax.broadcasted_iota(jnp.int32, shape, axis)


def slots(ids):
    tokens = ids.shape[1]
    named = jnp.sum((ids == 0).astype(F32), axis=0, keepdims=True)
    earlier = (iota((tokens, tokens), 0) < iota((tokens, tokens), 1)).astype(BF)
    wide = jnp.broadcast_to(named, (PACK, tokens))
    before = jnp.dot(wide.astype(BF), earlier, preferred_element_type=F32)
    slot = (iota((PACK, tokens), 0) % CAP).astype(F32)
    return jnp.where(before == slot, wide, 0.0)


def pack_kernel(*refs, grp_size, owners):
    sources, (rows_ref, slots_ref) = refs[:4], refs[4:6]
    held, done = refs[6:10], refs[10]
    loads = [
        pltpu.make_async_copy(source, target, done.at[n])
        for n, (source, target) in enumerate(zip(sources, held))
    ]
    for load in loads:
        load.start()
    for load in loads[:2]:
        load.wait()
    ids_ref, comb_ref, tok_ref, out_ref = held
    ids = ids_ref[...]
    both = slots(ids)
    slots_ref[...] = both
    model_width = tok_ref.shape[1]
    tokens = ids.shape[1]
    half = model_width // grp_size
    upper = iota((PACK, tokens), 0) < CAP
    first = jnp.where(upper, both, 0.0).astype(BF)
    second = jnp.where(upper, 0.0, both).astype(BF)
    chosen = jnp.sum(
        jnp.where(ids == 0, comb_ref[...].astype(F32), 0.0), axis=0, keepdims=True
    )
    scale = jnp.sum(both * chosen, axis=1, keepdims=True)
    scale = jnp.broadcast_to(scale, (PACK, LANES)).astype(BF)
    for load in loads[2:]:
        load.wait()
    packed = (
        jnp.dot(first, tok_ref[...], preferred_element_type=F32)
        + jnp.dot(second, out_ref[...], preferred_element_type=F32)
    ).astype(BF)
    width = model_width // owners
    for peer in range(rows_ref.shape[0]):
        side = peer % grp_size
        rows_ref[peer, :, :half] = packed[:, side * half : (side + 1) * half]
        rows_ref[peer, :, half : half + LANES] = scale
        for rep in range(owners // grp_size if rows_ref.shape[2] > half + LANES else 0):
            to = half + LANES + rep * width
            start = (rep * grp_size + side) * width
            rows_ref[peer, :, to : to + width] = packed[:, start : start + width]


def select_rows(recv_ref, first, depth, pick):
    peers = recv_ref.shape[0] // PACK
    block = 8 if peers % 8 == 0 else peers
    many = block * CAP
    row, col = iota((many, block * PACK), 0), iota((many, block * PACK), 1)
    take = (col == row // CAP * PACK + row % CAP + pick * CAP).astype(BF)
    for at in range(peers // block):
        piece = recv_ref[at * block * PACK : (at + 1) * block * PACK, first : first + depth]
        yield pl.ds(at * many, many), jnp.dot(take, piece, preferred_element_type=F32)


def forward_kernel(source_ref, far_ref, *refs, cut, first):
    own_ref, send_ref, near_ref = refs[:3]
    down_ref, done = refs[-2:]
    depth = far_ref.shape[1]
    piece = tile_of(depth, 256)
    pieces = [slice(at, at + piece) for at in range(0, depth, piece)]
    loads = []
    for n, here in enumerate(pieces):
        for k in range(3):
            target = down_ref if k == 2 else near_ref.at[k]
            loads.append(
                pltpu.make_async_copy(
                    far_ref.at[k, here, cut], target.at[here], done.at[3 * n + k]
                )
            )
    for load in loads:
        load.start()
    rows_ref = source_ref
    if first:
        rows_ref, scale_ref = refs[3:5]
        for here, xr in select_rows(source_ref, 0, depth + LANES, 0):
            rows_ref[0, here, :] = xr[:, :depth].astype(BF)
            scale_ref[here, :] = xr[:, depth:]
        for here, yr in select_rows(source_ref, 0, depth, 1):
            rows_ref[1, here, :] = yr.astype(BF)
        for cols_ref in refs[5:-2]:
            cols_ref[...] = source_ref[:, depth + LANES :]
    for n, here in enumerate(pieces):
        for k in range(3):
            loads[3 * n + k].wait()
            right_ref = down_ref if k == 2 else near_ref.at[k]
            part = jnp.dot(
                rows_ref[k // 2, :, here], right_ref[here], preferred_element_type=F32
            )
            if n:
                part = part + own_ref[k]
            own_ref[k] = part
            if n == len(pieces) - 1:
                send_ref[k] = part.astype(BF)


def hidden_kernel(own_ref, other_ref, scale_ref, *refs, tile, width):
    hid_ref, pc_ref = refs[-2 - bool(width) :][:2]
    if width:
        give_ref = refs[-1]
        keep, give = split_columns(*refs[:4], width)
        rows = hid_ref.shape[1]
        for held, target_ref in ((keep, hid_ref), (give, give_ref)):
            for at in range(len(held)):
                for part in range(2):
                    start = (part * len(held) + at) * width
                    piece = held[at][part * rows : (part + 1) * rows]
                    target_ref[3, :, start : start + width] = piece
    cr = scale_ref[:, :1]
    pc = jnp.zeros((scale_ref.shape[0], 1), F32)
    for start in range(0, hid_ref.shape[2], tile):
        here = slice(start, start + tile)
        a = own_ref[0, :, here] + other_ref[0, :, here].astype(F32)
        b = own_ref[1, :, here] + other_ref[1, :, here].astype(F32)
        back = own_ref[2, :, here] + other_ref[2, :, here].astype(F32)
        sig = jax.nn.sigmoid(a)
        act = a * sig
        h = act * b
        dh = cr * back
        made = (
            (dh * b * sig * (1.0 + a * (1.0 - sig))).astype(BF),
            (dh * act).astype(BF),
            (cr * h).astype(BF),
        )
        for k in range(3):
            hid_ref[k, :, here] = made[k]
            if width:
                give_ref[k, :, here] = made[k]
        pc = pc + jnp.sum(h * back, axis=1, keepdims=True)
    pc_ref[...] = jnp.broadcast_to(pc, pc_ref.shape)


def return_kernel(hid_ref, pc_ref, near_ref, *refs, first, last):
    contract = (((1,), (1,)), ((), ()))
    px = lax.dot_general(
        hid_ref[0], near_ref[0], contract, preferred_element_type=F32
    ) + lax.dot_general(hid_ref[1], near_ref[1], contract, preferred_element_type=F32)
    pc = pc_ref[...]
    if not first:
        px = px + refs[0][...]
        pc = pc + refs[1][...]
    if not last:
        refs[-2][...] = px
        refs[-1][...] = pc
        return
    back_ref = refs[-1]
    many = px.shape[0]
    half = px.shape[1] // 2
    low, high = px[:, :half], px[:, half:]
    upper = iota((many, half), 0) % PACK < CAP
    even = jnp.where(upper, low, pltpu.roll(high, CAP, 0))
    odd = jnp.where(upper, pltpu.roll(low, many - CAP, 0), high)
    pc_up = pltpu.roll(pc, many - CAP, 0)
    for q in range(many // PACK):
        at = slice(q * PACK, (q + 1) * PACK)
        back_ref[2 * q, :, :half] = even[at].astype(BF)
        back_ref[2 * q, :, half:] = pc[at].astype(BF)
        back_ref[2 * q + 1, :, :half] = odd[at].astype(BF)
        back_ref[2 * q + 1, :, half:] = pc_up[at].astype(BF)


def split_columns(rep_ref, grp_ref, near_ref, far_ref, width):
    blocks = near_ref.shape[1] // width // 2
    rep_high, grp = rep_ref[0] // blocks, grp_ref[0]
    keep, give = [], []

    def owned(ref, at, side):
        start = (2 * at + side) * width
        return ref[:, start : start + width]

    for at in range(blocks):
        mine = jnp.where(grp == 0, owned(near_ref, at, 0), owned(near_ref, at, 1))
        theirs = jnp.where(grp == 0, owned(far_ref, at, 0), owned(far_ref, at, 1))
        keep.append(jnp.where(rep_high == grp, mine, theirs))
        give.append(jnp.where(rep_high == grp, theirs, mine))
    return keep, give


def turn_kernel(rep_ref, *refs, many):
    cols_refs, (turned_ref, left_ref) = refs[:-2], refs[-2:]
    width = left_ref.shape[2]
    sources = many // CAP
    planes = len(cols_refs[0].shape) == 3
    if planes:
        block = sources // 2
        blocks = cols_refs[0].shape[2] // width // 2
    else:
        block = 8 if sources % 8 == 0 else sources
        blocks = cols_refs[0].shape[1] // width
    rows = block * CAP
    row, col = iota((rows, block * PACK), 0), iota((rows, block * PACK), 1)
    source = row // CAP * PACK + row % CAP
    take = [(col == source + k * CAP).astype(BF) for k in range(2)]

    def owned(ref, at, rep):
        if planes:
            start = (at * blocks + rep) * width
            return ref[3, :, start : start + width]
        here = slice(at * block * PACK, (at + 1) * block * PACK)
        return ref[here, rep * width : (rep + 1) * width]

    for m, cols_ref in enumerate(cols_refs):
        for at in range(sources // block):
            piece = owned(cols_ref, at, 0)
            for rep in range(1, blocks):
                piece = jnp.where(rep_ref[0] % blocks == rep, owned(cols_ref, at, rep), piece)
            for k in range(2):
                left_ref[k, pl.ds(m * many + at * rows, rows), :] = jnp.dot(
                    take[k], piece, preferred_element_type=F32
                )
    for k in range(2):
        turned_ref[k] = jnp.transpose(left_ref[k]).astype(BF)


def weight_kernel(turned_ref, *refs, cut, tile, members):
    hid_refs, (out_ref, made_ref, done) = refs[:members], refs[-3:]
    tiles = [
        (k, start) for start in range(0, cut.stop - cut.start, tile) for k in range(3)
    ]
    copies = [
        pltpu.make_async_copy(
            made_ref.at[k, :, pl.ds(start, tile)],
            out_ref.at[k, :, pl.ds(cut.start + start, tile)],
            done.at[n],
        )
        for n, (k, start) in enumerate(tiles)
    ]
    for n, (k, start) in enumerate(tiles):
        here = slice(start, start + tile)
        right = jnp.concatenate([ref[k, :, here] for ref in hid_refs], axis=0)
        made_ref[k, :, here] = jnp.dot(
            turned_ref[k // 2], right, preferred_element_type=F32
        )
        if n:
            copies[n - 1].start()
    copies[-1].start()
    for copy in copies:
        copy.wait()


def token_kernel(ids_ref, slots_ref, recv_ref, tok_ref, comb_ref, *, grp_size):
    both = slots_ref[...]
    peers = recv_ref.shape[0]
    tokens = both.shape[1]
    half = tok_ref.shape[1] // (2 * grp_size)
    upper = iota((PACK, tokens), 0) < CAP
    contract = (((0,), (0,)), ((), ()))
    picks = [
        jnp.where(upper, both, 0.0).astype(BF),
        jnp.where(upper, 0.0, both).astype(BF),
    ]
    for side in range(grp_size):
        total = recv_ref[side].astype(F32)
        for at in range(side + grp_size, peers, grp_size):
            total = total + recv_ref[at].astype(F32)
        if side == 0:
            pc = total[:, half:]
            per = jnp.sum(
                jnp.where(upper, both, 0.0) * pc[:, :1], axis=0, keepdims=True
            )
            comb_ref[...] = jnp.where(ids_ref[...] == 0, per, 0.0)
        rounded = total[:, :half].astype(BF)
        for part in range(2):
            start = (2 * side + part) * half
            tok_ref[:, start : start + half] = lax.dot_general(
                picks[part], rounded, contract, preferred_element_type=F32
            ).astype(BF)


def gather(piece, rep_size, give=None):
    pieces = [piece]
    step = rep_size // 2
    while step:
        pairs = [(i, i ^ step) for i in range(rep_size)]
        sent = [give] if give is not None and len(pieces) == 1 else pieces
        pieces = pieces + [lax.ppermute(held, "rep", pairs) for held in sent]
        step //= 2
    return pieces


def local(tokens, grad_out, expert_ids, combine, weights):
    ep_size = lax.axis_size("ep")
    rep_size = lax.axis_size("rep")
    grp_size = lax.axis_size("grp")
    token_count, model_width = tokens.shape
    peers = ep_size * grp_size
    many = peers * CAP
    depth, _, hidden = weights.shape
    owners = rep_size * grp_size
    owner_rows = model_width // owners
    tile = tile_of(hidden, 256)
    middle = -(-hidden // (2 * tile)) * tile
    cuts = [slice(0, hidden)]
    if middle < hidden:
        cuts = [slice(0, middle), slice(middle, hidden)]
    widths = [cut.stop - cut.start for cut in cuts]
    paired = grp_size == 2 and rep_size % 2 == 0 and widths[0] == rep_size * owner_rows
    side_width = depth + LANES + (0 if paired else rep_size * owner_rows)
    vmem = pl.BlockSpec(memory_space=pltpu.VMEM)
    hbm = pl.BlockSpec(memory_space=pltpu.HBM)
    ids = expert_ids.T
    w = jnp.transpose(weights, (1, 0, 2))

    rep = lax.axis_index("rep").astype(jnp.int32).reshape(1)
    grp = lax.axis_index("grp").astype(jnp.int32).reshape(1)
    ids, rep, grp = lax.optimization_barrier((ids, rep, grp))
    rows, slot_map = pl.pallas_call(
        functools.partial(pack_kernel, grp_size=grp_size, owners=owners),
        out_shape=(
            jax.ShapeDtypeStruct((peers, PACK, side_width), BF),
            jax.ShapeDtypeStruct((PACK, token_count), F32),
        ),
        in_specs=[hbm] * 4,
        out_specs=(vmem,) * 2,
        scratch_shapes=[
            pltpu.VMEM(ids.shape, ids.dtype),
            pltpu.VMEM(ids.shape, combine.dtype),
            pltpu.VMEM(tokens.shape, tokens.dtype),
            pltpu.VMEM(grad_out.shape, grad_out.dtype),
            pltpu.SemaphoreType.DMA((4,)),
        ],
        compiler_params=pltpu.CompilerParams(vmem_limit_bytes=WHOLE),
        cost_estimate=cost(2_000_000_000),
        name="pack",
    )(ids, combine.T, tokens, grad_out)

    recv = lax.all_to_all(rows, ("ep", "grp"), 0, 0, tiled=True)
    recv = recv.reshape(peers * PACK, side_width)

    far_recv = None
    if paired:
        far_recv = lax.ppermute(recv, "grp", [(0, 1), (1, 0)])

    source = recv
    owns, nears, others = [], [], []
    for c, width in enumerate(widths):
        first = c == 0
        extra = ()
        if first:
            extra = (
                jax.ShapeDtypeStruct((2, many, depth), BF),
                jax.ShapeDtypeStruct((many, LANES), F32),
            )
            if not paired:
                cols_shape = (peers * PACK, rep_size * owner_rows)
                extra += (jax.ShapeDtypeStruct(cols_shape, BF),)
        own, send, near, *more = pl.pallas_call(
            functools.partial(forward_kernel, cut=pl.ds(cuts[c].start, width), first=first),
            out_shape=(
                jax.ShapeDtypeStruct((3, many, width), F32),
                jax.ShapeDtypeStruct((3, many, width), BF),
                jax.ShapeDtypeStruct((2, depth, width), BF),
                *extra,
            ),
            in_specs=[vmem, hbm],
            out_specs=(vmem,) * (3 + len(extra)),
            scratch_shapes=[
                pltpu.VMEM((depth, width), BF),
                pltpu.SemaphoreType.DMA((3 * (depth // tile_of(depth, 256)),)),
            ],
            compiler_params=pltpu.CompilerParams(vmem_limit_bytes=WHOLE - (20 << 20)),
            cost_estimate=cost(3_000_000_000),
        )(source, w)
        if first:
            source, scale = more[:2]
            cols = more[2:]
        owns.append(own)
        nears.append(near)
        if grp_size == 2:
            others.append(lax.ppermute(send, "grp", [(0, 1), (1, 0)]))
        else:
            total = lax.psum(send.astype(F32), "grp")
            others.append((total - send.astype(F32)).astype(BF))

    gathered = []
    back = []
    for c, cut in enumerate(cuts):
        last = c == len(cuts) - 1
        fourth = paired and c == 0
        hid_shape = jax.ShapeDtypeStruct((3 + fourth, many, widths[c]), BF)
        smem = pl.BlockSpec(memory_space=pltpu.SMEM)
        hid, pc, *give = pl.pallas_call(
            functools.partial(hidden_kernel, tile=tile, width=owner_rows if fourth else 0),
            out_shape=(hid_shape, jax.ShapeDtypeStruct((many, LANES), F32))
            + (hid_shape,) * fourth,
            in_specs=[vmem] * 3 + [smem, smem, vmem, vmem] * fourth,
            out_specs=(vmem,) * (2 + fourth),
            compiler_params=pltpu.CompilerParams(vmem_limit_bytes=GRANT),
            cost_estimate=cost(1_000_000_000),
        )(owns[c], others[c], scale, *((rep, grp, recv, far_recv) * fourth))
        if last:
            shapes = jax.ShapeDtypeStruct((peers, PACK, depth // 2 + LANES), BF)
        else:
            shapes = (
                jax.ShapeDtypeStruct((many, depth), F32),
                jax.ShapeDtypeStruct((many, LANES), F32),
            )
        back = pl.pallas_call(
            functools.partial(return_kernel, first=c == 0, last=last),
            out_shape=shapes,
            in_specs=[vmem] * (3 + len(back)),
            out_specs=vmem if last else (vmem,) * 2,
            compiler_params=pltpu.CompilerParams(vmem_limit_bytes=GRANT),
            cost_estimate=cost(3_000_000_000),
        )(hid, pc, nears[c], *back)
        gathered.append(gather(hid, rep_size, *give))

    turned = pl.pallas_call(
        functools.partial(turn_kernel, many=many),
        out_shape=jax.ShapeDtypeStruct((2, owner_rows, rep_size * many), BF),
        in_specs=[smem] + [vmem] * rep_size,
        out_specs=vmem,
        scratch_shapes=[pltpu.VMEM((2, rep_size * many, owner_rows), F32)],
        compiler_params=pltpu.CompilerParams(vmem_limit_bytes=GRANT),
        cost_estimate=cost(500_000_000),
        name="turn",
    )(rep, *(gathered[0] if paired else gather(cols[0], rep_size)))

    back_recv = lax.all_to_all(back, ("ep", "grp"), 0, 0, tiled=True)

    grad_weights = []
    for c, cut in enumerate(cuts):
        grad_weights = [
            pl.pallas_call(
                functools.partial(weight_kernel, cut=cut, tile=tile, members=rep_size),
                out_shape=jax.ShapeDtypeStruct((3, owner_rows, hidden), F32),
                in_specs=[vmem] * (1 + rep_size)
                + [pl.BlockSpec(memory_space=pl.ANY)] * len(grad_weights),
                out_specs=pl.BlockSpec(memory_space=pl.ANY),
                scratch_shapes=[
                    pltpu.VMEM((3, owner_rows, widths[c]), F32),
                    pltpu.SemaphoreType.DMA((3 * (widths[c] // tile),)),
                ],
                input_output_aliases={1 + rep_size: 0} if grad_weights else {},
                compiler_params=pltpu.CompilerParams(vmem_limit_bytes=GRANT),
                cost_estimate=cost(3_000_000_000),
            )(turned, *gathered[c], *grad_weights)
        ]

    grad_tokens, grad_combine = pl.pallas_call(
        functools.partial(token_kernel, grp_size=grp_size),
        out_shape=(
            jax.ShapeDtypeStruct((token_count, model_width), BF),
            jax.ShapeDtypeStruct((2, token_count), F32),
        ),
        in_specs=[vmem] * 3,
        out_specs=(vmem,) * 2,
        compiler_params=pltpu.CompilerParams(vmem_limit_bytes=GRANT),
        cost_estimate=cost(2_000_000_000),
        name="token",
    )(ids, slot_map, back_recv)

    return (grad_tokens, grad_combine.T, jnp.transpose(grad_weights[0], (1, 0, 2)))


def solution(mesh):
    in_specs = (
        P(("rep", "ep", "grp"), None),
        P(("rep", "ep", "grp"), None),
        P(("rep", "ep", "grp"), None),
        P(("rep", "ep", "grp"), None),
        P("grp", None, "ep"),
    )
    out_specs = (
        P(("rep", "ep", "grp"), None),
        P(("rep", "ep", "grp"), None),
        P(("rep", "grp"), None, "ep"),
    )
    return jax.shard_map(
        local, mesh=mesh, in_specs=in_specs, out_specs=out_specs, check_vma=False
    )
```

```python
import functools

import jax
import jax.numpy as jnp
from jax import lax
from jax.experimental import pallas as pl
from jax.experimental.pallas import tpu as pltpu
from jax.sharding import PartitionSpec as P


CAP = 4
PACK = 2 * CAP
LANES = 128
GRANT = 16 << 20
WHOLE = 60 * 1024 * 1024
BF = jnp.bfloat16
F32 = jnp.float32


def tile_of(extent, most):
    for tile in range(most, 0, -LANES):
        if tile % LANES == 0 and extent % tile == 0:
            return tile
    return extent


def cost(flops):
    return pl.CostEstimate(flops=flops, bytes_accessed=0, transcendentals=0)


def iota(shape, axis):
    return lax.broadcasted_iota(jnp.int32, shape, axis)


def slots(ids):
    tokens = ids.shape[1]
    named = jnp.sum((ids == 0).astype(F32), axis=0, keepdims=True)
    earlier = (iota((tokens, tokens), 0) < iota((tokens, tokens), 1)).astype(BF)
    wide = jnp.broadcast_to(named, (PACK, tokens))
    before = jnp.dot(wide.astype(BF), earlier, preferred_element_type=F32)
    slot = (iota((PACK, tokens), 0) % CAP).astype(F32)
    return jnp.where(before == slot, wide, 0.0)


def pack_kernel(*refs, grp_size, owners, paired):
    grp_ref, *sources = refs[:5]
    made = 3 if paired else 2
    outs, (held, done) = refs[5 : 5 + made], (refs[5 + made : -1], refs[-1])
    loads = [
        pltpu.make_async_copy(source, target, done.at[n])
        for n, (source, target) in enumerate(zip(sources, held))
    ]
    for load in loads:
        load.start()
    for load in loads[:2]:
        load.wait()
    ids_ref, comb_ref, tok_ref, out_ref = held
    ids = ids_ref[...]
    both = slots(ids)
    outs[0][...] = both
    model_width = tok_ref.shape[1]
    tokens = ids.shape[1]
    half = model_width // grp_size
    width = model_width // owners
    reps = owners // grp_size
    upper = iota((PACK, tokens), 0) < CAP
    first = jnp.where(upper, both, 0.0).astype(BF)
    second = jnp.where(upper, 0.0, both).astype(BF)
    chosen = jnp.sum(
        jnp.where(ids == 0, comb_ref[...].astype(F32), 0.0), axis=0, keepdims=True
    )
    scale = jnp.sum(both * chosen, axis=1, keepdims=True)
    scale = jnp.broadcast_to(scale, (PACK, LANES)).astype(BF)
    for load in loads[2:]:
        load.wait()
    packed = (
        jnp.dot(first, tok_ref[...], preferred_element_type=F32)
        + jnp.dot(second, out_ref[...], preferred_element_type=F32)
    ).astype(BF)

    def owned(side, rep):
        start = (rep * grp_size + side) * width
        return packed[:, start : start + width]

    if not paired:
        rows_ref = outs[1]
        for peer in range(rows_ref.shape[0]):
            side = peer % grp_size
            rows_ref[peer, :, :half] = packed[:, side * half : (side + 1) * half]
            rows_ref[peer, :, half : half + LANES] = scale
            for rep in range(reps):
                to = half + LANES + rep * width
                rows_ref[peer, :, to : to + width] = owned(side, rep)
        return
    for to_ref, near, far in ((outs[1], 0, 1), (outs[2], 1, 0)):
        low = grp_ref[0] == 0
        to_ref[:, :half] = jnp.where(
            low, packed[:, near * half : (near + 1) * half], packed[:, far * half : (far + 1) * half]
        )
        to_ref[:, half : half + LANES] = scale
        for at in range(reps // 2):
            to = half + LANES + at * width
            to_ref[:, to : to + width] = jnp.where(
                low, owned(near, far * reps // 2 + at), owned(far, near * reps // 2 + at)
            )


def join_kernel(grp_ref, mine_ref, got_ref, out_ref):
    low = grp_ref[0] == 0
    out_ref[:PACK] = jnp.where(low, mine_ref[...], got_ref[...])
    out_ref[PACK:] = jnp.where(low, got_ref[...], mine_ref[...])


def select_rows(recv_ref, first, depth, pick):
    peers = recv_ref.shape[0] // PACK
    block = 8 if peers % 8 == 0 else peers
    many = block * CAP
    row, col = iota((many, block * PACK), 0), iota((many, block * PACK), 1)
    take = (col == row // CAP * PACK + row % CAP + pick * CAP).astype(BF)
    for at in range(peers // block):
        piece = recv_ref[at * block * PACK : (at + 1) * block * PACK, first : first + depth]
        yield pl.ds(at * many, many), jnp.dot(take, piece, preferred_element_type=F32)


def forward_kernel(*refs, inputs, cut, first):
    source_refs, w_ref, (own_ref, send_ref) = refs[:inputs], refs[inputs], refs[inputs + 1 :][:2]
    depth = w_ref.shape[1]
    rows_ref = source_refs[0]
    if first:
        rows_ref, scale_ref, recv_ref = refs[inputs + 3 :]
        many = recv_ref.shape[0] // inputs
        for m, source_ref in enumerate(source_refs):
            recv_ref[m * many : (m + 1) * many] = source_ref[...]
        for here, xr in select_rows(recv_ref, 0, depth + LANES, 0):
            rows_ref[0, here, :] = xr[:, :depth].astype(BF)
            scale_ref[here, :] = xr[:, depth:]
        for here, yr in select_rows(recv_ref, 0, depth, 1):
            rows_ref[1, here, :] = yr.astype(BF)
    for k in range(3):
        part = jnp.dot(rows_ref[k // 2], w_ref[k, :, cut], preferred_element_type=F32)
        own_ref[k] = part
        send_ref[k] = part.astype(BF)


def hidden_kernel(own_ref, other_ref, scale_ref, *refs, tile, width):
    hid_ref, pc_ref = refs[-2 - bool(width) :][:2]
    if width:
        give_ref = refs[-1]
        keep, give = split_columns(*refs[:3], width)
        rows = hid_ref.shape[1]
        for held, target_ref in ((keep, hid_ref), (give, give_ref)):
            for at in range(len(held)):
                for part in range(2):
                    start = (part * len(held) + at) * width
                    piece = held[at][part * rows : (part + 1) * rows]
                    target_ref[3, :, start : start + width] = piece
    cr = scale_ref[:, :1]
    pc = jnp.zeros((scale_ref.shape[0], 1), F32)
    for start in range(0, hid_ref.shape[2], tile):
        here = slice(start, start + tile)
        a = own_ref[0, :, here] + other_ref[0, :, here].astype(F32)
        b = own_ref[1, :, here] + other_ref[1, :, here].astype(F32)
        back = own_ref[2, :, here] + other_ref[2, :, here].astype(F32)
        sig = jax.nn.sigmoid(a)
        act = a * sig
        h = act * b
        dh = cr * back
        made = (
            (dh * b * sig * (1.0 + a * (1.0 - sig))).astype(BF),
            (dh * act).astype(BF),
            (cr * h).astype(BF),
        )
        for k in range(3):
            hid_ref[k, :, here] = made[k]
            if width:
                give_ref[k, :, here] = made[k]
        pc = pc + jnp.sum(h * back, axis=1, keepdims=True)
    pc_ref[...] = jnp.broadcast_to(pc, pc_ref.shape)


def return_kernel(ep_ref, hid_ref, pc_ref, w_ref, *refs, cut, first, last, near):
    contract = (((1,), (1,)), ((), ()))
    px = lax.dot_general(
        hid_ref[0], w_ref[0, :, cut], contract, preferred_element_type=F32
    ) + lax.dot_general(hid_ref[1], w_ref[1, :, cut], contract, preferred_element_type=F32)
    pc = pc_ref[...]
    if not first:
        px = px + refs[0][...]
        pc = pc + refs[1][...]
    if not last:
        refs[-2][...] = px
        refs[-1][...] = pc
        return
    back_ref = refs[-1]
    many = px.shape[0]
    half = px.shape[1] // 2
    low, high = px[:, :half], px[:, half:]
    upper = iota((many, half), 0) % PACK < CAP
    even = jnp.where(upper, low, pltpu.roll(high, CAP, 0))
    odd = jnp.where(upper, pltpu.roll(low, many - CAP, 0), high)
    pc_up = pltpu.roll(pc, many - CAP, 0)
    for q in range(many // PACK):
        at = slice(q * PACK, (q + 1) * PACK)
        to = 2 * (ep_ref[0] ^ q if near else q)
        back_ref[to, :, :half] = even[at].astype(BF)
        back_ref[to, :, half:] = pc[at].astype(BF)
        back_ref[to + 1, :, :half] = odd[at].astype(BF)
        back_ref[to + 1, :, half:] = pc_up[at].astype(BF)


def split_columns(rep_ref, grp_ref, recv_ref, width):
    blocks = (recv_ref.shape[1] - LANES) // 3 // width
    depth = 2 * blocks * width
    rep_high, grp = rep_ref[0] // blocks, grp_ref[0]
    keep, give = [], []
    for at in range(blocks):
        start = 2 * at * width
        near = jnp.where(
            grp == 0,
            recv_ref[:, start : start + width],
            recv_ref[:, start + width : start + 2 * width],
        )
        start = depth + LANES + at * width
        far = recv_ref[:, start : start + width]
        keep.append(jnp.where(rep_high == grp, near, far))
        give.append(jnp.where(rep_high == grp, far, near))
    return keep, give


def turn_kernel(rep_ref, *refs, many):
    cols_refs, (turned_ref, left_ref) = refs[:-2], refs[-2:]
    width = left_ref.shape[2]
    sources = many // CAP
    planes = len(cols_refs[0].shape) == 3
    if planes:
        block = sources // 2
        blocks = cols_refs[0].shape[2] // width // 2
    else:
        block = 8 if sources % 8 == 0 else sources
        blocks = cols_refs[0].shape[1] // width
    rows = block * CAP
    row, col = iota((rows, block * PACK), 0), iota((rows, block * PACK), 1)
    source = row // CAP * PACK + row % CAP
    take = [(col == source + k * CAP).astype(BF) for k in range(2)]

    def owned(ref, at, rep):
        if planes:
            start = (at * blocks + rep) * width
            return ref[3, :, start : start + width]
        here = slice(at * block * PACK, (at + 1) * block * PACK)
        return ref[here, rep * width : (rep + 1) * width]

    for m, cols_ref in enumerate(cols_refs):
        for at in range(sources // block):
            piece = owned(cols_ref, at, 0)
            for rep in range(1, blocks):
                piece = jnp.where(rep_ref[0] % blocks == rep, owned(cols_ref, at, rep), piece)
            for k in range(2):
                left_ref[k, pl.ds(m * many + at * rows, rows), :] = jnp.dot(
                    take[k], piece, preferred_element_type=F32
                )
    for k in range(2):
        turned_ref[k] = jnp.transpose(left_ref[k]).astype(BF)


def weight_kernel(turned_ref, *refs, cut, tile, members):
    hid_refs, (out_ref, made_ref, done) = refs[:members], refs[-3:]
    tiles = [
        (k, start) for start in range(0, cut.stop - cut.start, tile) for k in range(3)
    ]
    copies = [
        pltpu.make_async_copy(
            made_ref.at[k, :, pl.ds(start, tile)],
            out_ref.at[k, :, pl.ds(cut.start + start, tile)],
            done.at[n],
        )
        for n, (k, start) in enumerate(tiles)
    ]
    for n, (k, start) in enumerate(tiles):
        here = slice(start, start + tile)
        right = jnp.concatenate([ref[k, :, here] for ref in hid_refs], axis=0)
        made_ref[k, :, here] = jnp.dot(
            turned_ref[k // 2], right, preferred_element_type=F32
        )
        if n:
            copies[n - 1].start()
    copies[-1].start()
    for copy in copies:
        copy.wait()


def token_kernel(ids_ref, slots_ref, recv_ref, tok_ref, comb_ref, *, grp_size):
    both = slots_ref[...]
    peers = recv_ref.shape[0]
    tokens = both.shape[1]
    half = tok_ref.shape[1] // (2 * grp_size)
    upper = iota((PACK, tokens), 0) < CAP
    contract = (((0,), (0,)), ((), ()))
    picks = [
        jnp.where(upper, both, 0.0).astype(BF),
        jnp.where(upper, 0.0, both).astype(BF),
    ]
    for side in range(grp_size):
        total = recv_ref[side].astype(F32)
        for at in range(side + grp_size, peers, grp_size):
            total = total + recv_ref[at].astype(F32)
        if side == 0:
            pc = total[:, half:]
            per = jnp.sum(
                jnp.where(upper, both, 0.0) * pc[:, :1], axis=0, keepdims=True
            )
            comb_ref[...] = jnp.where(ids_ref[...] == 0, per, 0.0)
        rounded = total[:, :half].astype(BF)
        for part in range(2):
            start = (2 * side + part) * half
            tok_ref[:, start : start + half] = lax.dot_general(
                picks[part], rounded, contract, preferred_element_type=F32
            ).astype(BF)


def gather(piece, rep_size, give=None):
    pieces = [piece]
    step = rep_size // 2
    while step:
        pairs = [(i, i ^ step) for i in range(rep_size)]
        sent = [give] if give is not None and len(pieces) == 1 else pieces
        pieces = pieces + [lax.ppermute(held, "rep", pairs) for held in sent]
        step //= 2
    return pieces


def local(tokens, grad_out, expert_ids, combine, weights):
    ep_size = lax.axis_size("ep")
    rep_size = lax.axis_size("rep")
    grp_size = lax.axis_size("grp")
    token_count, model_width = tokens.shape
    peers = ep_size * grp_size
    many = peers * CAP
    depth, _, hidden = weights.shape
    owners = rep_size * grp_size
    owner_rows = model_width // owners
    tile = tile_of(hidden, 256)
    middle = -(-hidden // (2 * tile)) * tile
    cuts = [slice(0, hidden)]
    if middle < hidden:
        cuts = [slice(0, middle), slice(middle, hidden)]
    widths = [cut.stop - cut.start for cut in cuts]
    paired = grp_size == 2 and ep_size == 4 and rep_size % 2 == 0
    paired = paired and widths[0] == rep_size * owner_rows == depth
    side_width = depth + LANES + rep_size * owner_rows // (2 if paired else 1)
    vmem = pl.BlockSpec(memory_space=pltpu.VMEM)
    hbm = pl.BlockSpec(memory_space=pltpu.HBM)
    ids = expert_ids.T
    w = jnp.transpose(weights, (1, 0, 2))

    smem = pl.BlockSpec(memory_space=pltpu.SMEM)
    rep = lax.axis_index("rep").astype(jnp.int32).reshape(1)
    ep = lax.axis_index("ep").astype(jnp.int32).reshape(1)
    grp = lax.axis_index("grp").astype(jnp.int32).reshape(1)
    ids, rep, ep, grp = lax.optimization_barrier((ids, rep, ep, grp))
    if paired:
        row_shapes = (jax.ShapeDtypeStruct((PACK, side_width), BF),) * 2
    else:
        row_shapes = (jax.ShapeDtypeStruct((peers, PACK, side_width), BF),)
    slot_map, *rows = pl.pallas_call(
        functools.partial(pack_kernel, grp_size=grp_size, owners=owners, paired=paired),
        out_shape=(jax.ShapeDtypeStruct((PACK, token_count), F32), *row_shapes),
        in_specs=[smem] + [hbm] * 4,
        out_specs=(vmem,) * (1 + len(row_shapes)),
        scratch_shapes=[
            pltpu.VMEM(ids.shape, ids.dtype),
            pltpu.VMEM(ids.shape, combine.dtype),
            pltpu.VMEM(tokens.shape, tokens.dtype),
            pltpu.VMEM(grad_out.shape, grad_out.dtype),
            pltpu.SemaphoreType.DMA((4,)),
        ],
        compiler_params=pltpu.CompilerParams(vmem_limit_bytes=WHOLE),
        cost_estimate=cost(2_000_000_000),
        name="pack",
    )(grp, ids, combine.T, tokens, grad_out)

    if paired:
        got = lax.ppermute(rows[1], "grp", [(0, 1), (1, 0)])
        joined = pl.pallas_call(
            join_kernel,
            out_shape=jax.ShapeDtypeStruct((grp_size * PACK, side_width), BF),
            in_specs=[smem] + [vmem] * 2,
            out_specs=vmem,
            compiler_params=pltpu.CompilerParams(vmem_limit_bytes=GRANT),
            cost_estimate=cost(3_000_000_000),
            name="join",
        )(grp, rows[0], got)
        sources = [joined]
        for flip in range(1, ep_size):
            pairs = [(i, i ^ flip) for i in range(ep_size)]
            sources.append(lax.ppermute(joined, "ep", pairs))
    else:
        recv = lax.all_to_all(rows[0], ("ep", "grp"), 0, 0, tiled=True)
        sources = [recv.reshape(peers * PACK, side_width)]

    owns, others = [], []
    for c, width in enumerate(widths):
        first = c == 0
        extra = ()
        if first:
            extra = (
                jax.ShapeDtypeStruct((2, many, depth), BF),
                jax.ShapeDtypeStruct((many, LANES), F32),
                jax.ShapeDtypeStruct((peers * PACK, side_width), BF),
            )
        own, send, *more = pl.pallas_call(
            functools.partial(forward_kernel, inputs=len(sources), cut=cuts[c], first=first),
            out_shape=(
                jax.ShapeDtypeStruct((3, many, width), F32),
                jax.ShapeDtypeStruct((3, many, width), BF),
                *extra,
            ),
            in_specs=[vmem] * (len(sources) + 1),
            out_specs=(vmem,) * (2 + len(extra)),
            compiler_params=pltpu.CompilerParams(vmem_limit_bytes=GRANT),
            cost_estimate=cost(3_000_000_000),
        )(*sources, w)
        if first:
            source, scale, recv = more
            sources = [source]
        owns.append(own)
        if grp_size == 2:
            others.append(lax.ppermute(send, "grp", [(0, 1), (1, 0)]))
        else:
            total = lax.psum(send.astype(F32), "grp")
            others.append((total - send.astype(F32)).astype(BF))

    gathered = []
    back = []
    for c, cut in enumerate(cuts):
        last = c == len(cuts) - 1
        fourth = paired and c == 0
        hid_shape = jax.ShapeDtypeStruct((3 + fourth, many, widths[c]), BF)
        hid, pc, *give = pl.pallas_call(
            functools.partial(hidden_kernel, tile=tile, width=owner_rows if fourth else 0),
            out_shape=(hid_shape, jax.ShapeDtypeStruct((many, LANES), F32))
            + (hid_shape,) * fourth,
            in_specs=[vmem] * 3 + [smem, smem, vmem] * fourth,
            out_specs=(vmem,) * (2 + fourth),
            compiler_params=pltpu.CompilerParams(vmem_limit_bytes=GRANT),
            cost_estimate=cost(1_000_000_000),
        )(owns[c], others[c], scale, *((rep, grp, recv) * fourth))
        if last:
            shapes = jax.ShapeDtypeStruct((peers, PACK, depth // 2 + LANES), BF)
        else:
            shapes = (
                jax.ShapeDtypeStruct((many, depth), F32),
                jax.ShapeDtypeStruct((many, LANES), F32),
            )
        back = pl.pallas_call(
            functools.partial(
                return_kernel, cut=cut, first=c == 0, last=last, near=paired
            ),
            out_shape=shapes,
            in_specs=[smem] + [vmem] * (3 + len(back)),
            out_specs=vmem if last else (vmem,) * 2,
            compiler_params=pltpu.CompilerParams(vmem_limit_bytes=GRANT),
            cost_estimate=cost(3_000_000_000),
        )(ep, hid, pc, w, *back)
        gathered.append(gather(hid, rep_size, *give))

    turned = pl.pallas_call(
        functools.partial(turn_kernel, many=many),
        out_shape=jax.ShapeDtypeStruct((2, owner_rows, rep_size * many), BF),
        in_specs=[smem] + [vmem] * rep_size,
        out_specs=vmem,
        scratch_shapes=[pltpu.VMEM((2, rep_size * many, owner_rows), F32)],
        compiler_params=pltpu.CompilerParams(vmem_limit_bytes=GRANT),
        cost_estimate=cost(500_000_000),
        name="turn",
    )(rep, *(gathered[0] if paired else gather(recv[:, depth + LANES :], rep_size)))

    back_recv = lax.all_to_all(back, ("ep", "grp"), 0, 0, tiled=True)

    grad_weights = []
    for c, cut in enumerate(cuts):
        grad_weights = [
            pl.pallas_call(
                functools.partial(weight_kernel, cut=cut, tile=tile, members=rep_size),
                out_shape=jax.ShapeDtypeStruct((3, owner_rows, hidden), F32),
                in_specs=[vmem] * (1 + rep_size)
                + [pl.BlockSpec(memory_space=pl.ANY)] * len(grad_weights),
                out_specs=pl.BlockSpec(memory_space=pl.ANY),
                scratch_shapes=[
                    pltpu.VMEM((3, owner_rows, widths[c]), F32),
                    pltpu.SemaphoreType.DMA((3 * (widths[c] // tile),)),
                ],
                input_output_aliases={1 + rep_size: 0} if grad_weights else {},
                compiler_params=pltpu.CompilerParams(vmem_limit_bytes=GRANT),
                cost_estimate=cost(3_000_000_000),
            )(turned, *gathered[c], *grad_weights)
        ]

    grad_tokens, grad_combine = pl.pallas_call(
        functools.partial(token_kernel, grp_size=grp_size),
        out_shape=(
            jax.ShapeDtypeStruct((token_count, model_width), BF),
            jax.ShapeDtypeStruct((2, token_count), F32),
        ),
        in_specs=[vmem] * 3,
        out_specs=(vmem,) * 2,
        compiler_params=pltpu.CompilerParams(vmem_limit_bytes=GRANT),
        cost_estimate=cost(2_000_000_000),
        name="token",
    )(ids, slot_map, back_recv)

    return (grad_tokens, grad_combine.T, jnp.transpose(grad_weights[0], (1, 0, 2)))


def solution(mesh):
    in_specs = (
        P(("rep", "ep", "grp"), None),
        P(("rep", "ep", "grp"), None),
        P(("rep", "ep", "grp"), None),
        P(("rep", "ep", "grp"), None),
        P("grp", None, "ep"),
    )
    out_specs = (
        P(("rep", "ep", "grp"), None),
        P(("rep", "ep", "grp"), None),
        P(("rep", "grp"), None, "ep"),
    )
    return jax.shard_map(local, mesh=mesh, in_specs=in_specs, out_specs=out_specs, check_vma=False)
```
